256 devices in a mesh: curve: 64 (over y, z, core), sub: 4 (over x).
Axes of the slice: x: 4, y: 4, z: 8, core: 2. Of those that a mesh axis runs over, the one named last changes fastest.
Arguments:
- forcing: float32 [12, 6144, 1024], P(None, 'curve', 'sub'), may hold values from -10 to 10
- metric: float32 [6144, 1024], P('curve', 'sub'), may hold values from 0.25 to 4
- jacobian: float32 [6144, 1024], P('curve', 'sub'), may hold values from 0.5 to 2
- mode_scale: float32 [12], replicated, may hold values from 0.1 to 10
Outputs:
- solution: float32 [12, 6144, 1024], P(None, 'curve', 'sub')
- residual: float32 [12, 6144, 1024], P(None, 'curve', 'sub')
The draws below stay inside these ranges and needn't reach their ends.
All inputs are finite; a program needn't handle non-finite values.
Results may differ from the reference program's by a relative error of at most 0.0003.
Values sent between devices are 32-bit elements; how exact they have to be, the bound alone decides.
A program may use at most 64 MiB of HBM per device.

```python
import math
import jax
import jax.numpy as jnp
import numpy as np
from jax import lax

NP = 4
MODES = 12
ITERS = 3
EBX = 24
NX = 6144
NY = 1024


def draw_forcing(key, part):
    noise_key, scale_key = jax.random.split(jax.random.fold_in(key, 7))
    regions = NX // (NP * EBX)
    region_scale = jnp.exp(jax.random.uniform(scale_key, (regions,), jnp.float32, math.log(0.3), math.log(3.0)))
    per_row = jnp.repeat(region_scale, NP * EBX)
    base = jax.random.normal(noise_key, (MODES, NX, NY), jnp.float32)
    return jnp.clip(base * per_row[None, :, None], -10.0, 10.0)


def block_scale(key, extent, cuts, low, high):
    level, own = 1.0, jax.random.fold_in(key, 6)
    for axis_at, blocks in cuts:
        steps = jnp.exp(jax.random.uniform(jax.random.fold_in(own, axis_at), (blocks,), jnp.float32, low / len(cuts), high / len(cuts)))
        level = level * jnp.repeat(steps, extent[axis_at] // blocks).reshape([-1 if axis == axis_at else 1 for axis in range(len(extent))])
    return level


def setup_inputs(seed: int = 0) -> dict:
    key_list = jax.random.split(jax.random.key(seed), 5)
    forcing = draw_forcing(jax.random.fold_in(key_list[4], 71), 0)
    metric = jnp.clip(jnp.exp(math.log(4.0) - 2.7725887 * jax.random.uniform(key_list[1], (NX, NY), jnp.float32) ** block_scale(key_list[1], (NX, NY), ((0, 64), (1, 4)), -0.2, 0.2)), 0.25, 4.0)
    jacobian = jnp.clip(jnp.exp(math.log(2.0) - 1.3862944 * jax.random.uniform(key_list[2], (NX, NY), jnp.float32) ** block_scale(key_list[2], (NX, NY), ((0, 64), (1, 4)), -0.2, 0.2)), 0.5, 2.0)
    mode_scale = jnp.clip(jnp.exp(jax.random.uniform(key_list[3], (MODES,), jnp.float32, math.log(0.1), math.log(10.0))), 0.1, 10.0)
    return {"forcing": forcing, "metric": metric, "jacobian": jacobian, "mode_scale": mode_scale}


def gll_tables():
    points = np.array([-1.0, -1.0 / math.sqrt(5.0), 1.0 / math.sqrt(5.0), 1.0])
    weights = np.array([1.0 / 6.0, 5.0 / 6.0, 5.0 / 6.0, 1.0 / 6.0])
    factor = np.array([np.prod([points[j] - points[m] for m in range(4) if m != j]) for j in range(4)])
    slopes = np.zeros((4, 4))
    for i in range(4):
        for j in range(4):
            if i != j:
                slopes[i, j] = factor[i] / (factor[j] * (points[i] - points[j]))
        slopes[i, i] = sum((1.0 / (points[i] - points[m]) for m in range(4) if m != i))
    return (slopes, weights)

def line_tables(count):
    phase = jnp.arange(count, dtype=jnp.int32) % 4
    on_edge = (phase == 0) | (phase == 3)
    line_w = jnp.where(on_edge, jnp.float32(1.0 / 6.0), jnp.float32(5.0 / 6.0))
    line_mult = jnp.where(on_edge, jnp.float32(2.0), jnp.float32(1.0))
    return (line_w, line_mult)

def assemble(values):
    for axis_dim in (0, 1):
        phase = lax.broadcasted_iota(jnp.int32, values.shape, axis_dim) % 4
        values = values + jnp.where(phase == 3, jnp.roll(values, -1, axis_dim), 0.0) + jnp.where(phase == 0, jnp.roll(values, 1, axis_dim), 0.0)
    return values

def apply_local(values, scale, slopes, mass_w, flux_w):
    row_count, col_count = values.shape
    shape4 = (row_count // 4, 4, col_count // 4, 4)
    blocks = values.reshape(shape4)
    hp = lax.Precision.HIGHEST
    grad_x = jnp.einsum('ak,xkyb->xayb', slopes, blocks, precision=hp)
    grad_y = jnp.einsum('bk,xayk->xayb', slopes, blocks, precision=hp)
    weight4 = flux_w.reshape(shape4)
    lap = jnp.einsum('ka,xkyb->xayb', slopes, weight4 * grad_x, precision=hp) + jnp.einsum('kb,xayk->xayb', slopes, weight4 * grad_y, precision=hp)
    return mass_w * values + scale * lap.reshape(row_count, col_count)

def diag_terms(flux_w, slopes):
    row_count, col_count = flux_w.shape
    shape4 = (row_count // 4, 4, col_count // 4, 4)
    weight4 = flux_w.reshape(shape4)
    hp = lax.Precision.HIGHEST
    squared = slopes * slopes
    terms = jnp.einsum('ka,xkyb->xayb', squared, weight4, precision=hp) + jnp.einsum('kb,xayk->xayb', squared, weight4, precision=hp)
    return terms.reshape(row_count, col_count)

def reference(forcing, metric, jacobian, mode_scale):
    slopes = jnp.asarray(gll_tables()[0], jnp.float32)
    row_w, row_mult = line_tables(metric.shape[0])
    col_w, col_mult = line_tables(metric.shape[1])
    grid_w = row_w[:, None] * col_w[None, :]
    inv_count = 1.0 / (row_mult[:, None] * col_mult[None, :])
    mass_w = jacobian * grid_w
    flux_w = metric * grid_w
    mass_diag = assemble(mass_w)
    lap_diag = assemble(diag_terms(flux_w, slopes))

    def solve_mode(member):
        source, scale = member
        rhs = assemble(source * mass_w)
        precond = mass_diag + scale * lap_diag
        solution = jnp.zeros_like(rhs)
        residual = rhs
        zvec = residual / precond
        direction = zvec
        rho_now = jnp.sum(residual * zvec * inv_count)
        for iteration in range(ITERS):
            image = assemble(apply_local(direction, scale, slopes, mass_w, flux_w))
            step_len = rho_now / jnp.sum(direction * image * inv_count)
            solution = solution + step_len * direction
            residual = residual - step_len * image
            zvec = residual / precond
            rho_next = jnp.sum(residual * zvec * inv_count)
            direction = zvec + rho_next / rho_now * direction
            rho_now = rho_next
        return (solution, residual)
    solution, residual = lax.map(solve_mode, (forcing, mode_scale))
    return (solution, residual)
```

```python
import functools
import math

import jax
import jax.numpy as jnp
import numpy as np
from jax import lax
from jax.experimental import pallas as pl
from jax.experimental.pallas import tpu as pltpu
from jax.sharding import PartitionSpec as P

MESH = pl.DeviceIdType.MESH
EDGES = ((0, 1), (0, 2), (0, 3), (1, 2), (1, 3), (2, 3))
F32 = jnp.float32


def gll_slopes():
    points = np.array([-1.0, -1.0 / math.sqrt(5.0), 1.0 / math.sqrt(5.0), 1.0])
    factor = np.array(
        [np.prod([points[j] - points[m] for m in range(4) if m != j]) for j in range(4)]
    )
    slopes = np.zeros((4, 4))
    for i in range(4):
        for j in range(4):
            if i != j:
                slopes[i, j] = factor[i] / (factor[j] * (points[i] - points[j]))
        slopes[i, i] = sum((1.0 / (points[i] - points[m]) for m in range(4) if m != i))
    return slopes


def kernel(
    cfg,
    scale_ref,
    f_hbm,
    met_hbm,
    jac_hbm,
    x_ref,
    r_ref,
    fbuf,
    metbuf,
    jacbuf,
    w0,
    w1,
    w2,
    w3,
    y0,
    y1,
    y2,
    minv,
    mass,
    cx,
    cy,
    dots,
    rowbuf,
    colbuf,
    rowrecv,
    cornrecv,
    colrecv,
    rowfix,
    colfix,
    red,
    in_sems,
    send_sems,
    recv_sems,
    rs_send,
    rs_recv,
):
    n_modes, n_curve, n_sub, n_zc = cfg
    n_y = n_curve // n_zc
    c = lax.axis_index("curve")
    s = lax.axis_index("sub")
    c_prev, c_next = lax.rem(c + n_curve - 1, n_curve), lax.rem(c + 1, n_curve)
    s_prev, s_next = lax.rem(s + n_sub - 1, n_sub), lax.rem(s + 1, n_sub)
    y_pos, zc_pos = c // n_zc, lax.rem(c, n_zc)
    b_size = n_y * n_sub
    b_pos = y_pos * n_sub + s

    halves = (pl.ds(0, 128), pl.ds(128, 128))
    loads = []
    for h in range(2):
        loads.append(pltpu.make_async_copy(met_hbm.at[:, halves[h]], metbuf.at[h], in_sems.at[0, h]))
        loads.append(pltpu.make_async_copy(jac_hbm.at[:, halves[h]], jacbuf.at[h], in_sems.at[1, h]))
    for m in range(n_modes):
        for h in range(2):
            loads.append(
                pltpu.make_async_copy(f_hbm.at[m, :, halves[h]], fbuf.at[m, h], in_sems.at[2 + m, h])
            )
    for load in loads:
        load.start()

    def a_member(d):
        pos = lax.rem(zc_pos + d, n_zc)
        return (y_pos * n_zc + pos, s)

    def b_member(d):
        pos = lax.rem(b_pos + d, b_size)
        return ((pos // n_sub) * n_zc + zc_pos, lax.rem(pos, n_sub))

    around = [
        (c_prev, s), (c_next, s), (c, s_prev), (c, s_next),
        (c_prev, s_prev), (c_prev, s_next), (c_next, s_prev), (c_next, s_next),
    ]
    partners = around + [a_member(d) for d in range(1, n_zc)] + [b_member(d) for d in range(1, b_size)]
    barrier = pltpu.get_barrier_semaphore()
    for device in partners:
        pl.semaphore_signal(barrier, inc=1, device_id=device, device_id_type=MESH)

    lane = lax.broadcasted_iota(jnp.int32, (8, 128), 1)
    subl = lax.broadcasted_iota(jnp.int32, (8, 128), 0)
    phase = lane & 3
    lane24 = lax.broadcasted_iota(jnp.int32, (24, 128), 1)
    row24 = lax.broadcasted_iota(jnp.int32, (24, 256), 0)
    slopes = gll_slopes()

    def by_phase(values):
        out = jnp.full((8, 128), F32(values[3]))
        for b in (2, 1, 0):
            out = jnp.where(phase == b, F32(values[b]), out)
        return out

    def block(t):
        return pl.multiple_of((t // 2) * 8, 8), pl.multiple_of(lax.rem(t, 2) * 128, 128)

    def natural(r0, a):
        return pl.ds(a + 4 * r0, 8, stride=4)

    weights = (1.0 / 6.0, 5.0 / 6.0, 5.0 / 6.0, 1.0 / 6.0)
    col_w = by_phase(weights)
    col_count = by_phase((0.5, 1.0, 1.0, 0.5))

    def coupling(d, shift):
        vals = []
        for b in range(4):
            ok = 0 <= b + shift < 4 and b + d < 4
            vals.append(slopes[b + shift, b] * slopes[b + shift, b + d] if ok else 0.0)
        return by_phase(vals)

    for load in loads[:4]:
        load.wait()
    shifts = range(-3, 4)
    pair_tab = {(d, q): coupling(d, q) for d in (0, 1, 2, 3) for q in shifts}

    def setup(t, carry):
        r0, l0 = block(t)
        rows, cols = pl.ds(r0, 8), pl.ds(l0, 128)
        flux = []
        for a in range(4):
            grid_w = col_w * F32(weights[a])
            m_a = jacbuf[l0 // 128, natural(r0, a), :] * grid_w
            mass[a, rows, cols] = m_a
            w0[n_modes, a, rows, cols] = m_a
            flux.append(metbuf[l0 // 128, natural(r0, a), :] * grid_w)
        for e, (i, j) in enumerate(EDGES):
            total = flux[0] * F32(slopes[0, i] * slopes[0, j])
            for q in range(1, 4):
                total = total + flux[q] * F32(slopes[q, i] * slopes[q, j])
            cx[e, rows, cols] = total
        for a in range(4):
            rolled = {q: flux[a] if q == 0 else pltpu.roll(flux[a], (-q) % 128, 1) for q in shifts}
            lap = flux[0] * F32(slopes[0, a] ** 2)
            for q in range(1, 4):
                lap = lap + flux[q] * F32(slopes[q, a] ** 2)
            for q in shifts:
                lap = lap + rolled[q] * pair_tab[0, q]
            w0[n_modes + 1, a, rows, cols] = lap
            for d in (1, 2, 3):
                total = None
                for q in range(-3, 4):
                    if not any(0 <= b + q < 4 and b + d < 4 for b in range(4)):
                        continue
                    term = rolled[q] * pair_tab[d, q]
                    total = term if total is None else total + term
                cy[d - 1, a, rows, cols] = total
        return carry

    lax.fori_loop(0, 6, setup, 0)
    for load in loads[4:]:
        load.wait()

    def weigh(t, carry):
        r0, l0 = block(t)
        rows, cols = pl.ds(r0, 8), pl.ds(l0, 128)
        for a in range(4):
            m_a = mass[a, rows, cols]
            for m in range(n_modes):
                w0[m, a, rows, cols] = fbuf[m, l0 // 128, natural(r0, a), :] * m_a
        return carry

    lax.fori_loop(0, 6, weigh, 0)
    dots[...] = jnp.zeros_like(dots)

    def row_join_and_pack(e, w, count):
        packed = jnp.zeros((24, 128), F32)
        for m in range(count):
            top, bottom = w[m, 0], w[m, 3]
            bottom = bottom + jnp.where(row24 < 23, pltpu.roll(top, 23, 0), 0.0)
            top = jnp.where(row24 > 0, pltpu.roll(bottom, 1, 0), top)
            w[m, 0] = top
            w[m, 3] = bottom
            rowbuf[e, 0, m : m + 1, :] = top[0:1, :]
            rowbuf[e, 1, m : m + 1, :] = bottom[23:24, :]
            for a, plane in enumerate((top, w[m, 1], w[m, 2], bottom)):
                k = 4 * m + a
                ends = jnp.where(lane24 == 127, plane[:, 128:], plane[:, :128])
                ends = pltpu.roll(ends, 2 * k, 1) if k else ends
                packed = jnp.where(
                    (lane24 == 2 * k) | (lane24 == (2 * k - 1) % 128), ends, packed
                )
        colbuf[e] = packed

    def copies(e):
        low, high = pl.ds(0, 128), pl.ds(128, 128)
        plan = [
            (rowbuf.at[e, 1], rowrecv.at[e, 0], (c_next, s)),
            (rowbuf.at[e, 0], rowrecv.at[e, 1], (c_prev, s)),
            (colbuf.at[e], colrecv.at[e, 0], (c, s_next)),
            (colbuf.at[e], colrecv.at[e, 1], (c, s_prev)),
            (rowbuf.at[e, 1, :, high], cornrecv.at[e, 0], (c_next, s_next)),
            (rowbuf.at[e, 1, :, low], cornrecv.at[e, 1], (c_next, s_prev)),
            (rowbuf.at[e, 0, :, high], cornrecv.at[e, 2], (c_prev, s_next)),
            (rowbuf.at[e, 0, :, low], cornrecv.at[e, 3], (c_prev, s_prev)),
        ]
        return [
            pltpu.make_async_remote_copy(
                src_ref=src,
                dst_ref=dst,
                send_sem=send_sems.at[e, i],
                recv_sem=recv_sems.at[e, i],
                device_id=device,
                device_id_type=MESH,
            )
            for i, (src, dst, device) in enumerate(plan)
        ]

    def col_join(plane):
        lanes = lax.broadcasted_iota(jnp.int32, (plane.shape[0], 128), 1)
        last, first = lanes == 127, lanes == 0
        high_end, low_end = (lanes & 3) == 3, (lanes & 3) == 0
        x0, x1 = plane[:, :128], plane[:, 128:]
        n0, n1 = pltpu.roll(x0, 127, 1), pltpu.roll(x1, 127, 1)
        s0 = x0 + jnp.where(last, n1, n0)
        s1 = x1 + jnp.where(last, 0.0, n1)
        p0, p1 = pltpu.roll(s0, 1, 1), pltpu.roll(s1, 1, 1)
        out0 = jnp.where(high_end, s0, jnp.where(low_end, jnp.where(first, x0, p0), x0))
        out1 = jnp.where(high_end, s1, jnp.where(low_end, jnp.where(first, p0, p1), x1))
        return out0, out1

    def exchange(e, w, count):
        row_join_and_pack(e, w, count)
        if e == 0:
            pl.semaphore_wait(barrier, len(partners))
        sent = copies(e)
        for copy in sent:
            copy.start()
        for m in range(count):
            for a in range(4):
                out0, out1 = col_join(w[m, a])
                w[m, a, :, 0:128] = out0
                w[m, a, :, 128:256] = out1
        return sent

    def arrive(e, sent):
        for copy in sent:
            copy.wait_recv()
        lanes = lax.broadcasted_iota(jnp.int32, (16, 128), 1)
        for side in range(2):
            out0, out1 = col_join(rowrecv[e, side])
            left = pltpu.roll(cornrecv[e, 2 * side], 1, 1)
            right = pltpu.roll(cornrecv[e, 2 * side + 1], 127, 1)
            rowfix[side, :, 0:128] = out0 + jnp.where(lanes == 0, left, 0.0)
            rowfix[side, :, 128:256] = out1 + jnp.where(lanes == 127, right, 0.0)
        colfix[...] = jnp.where(
            (lane24 & 1) == 0, pltpu.roll(colrecv[e, 0], 1, 1), pltpu.roll(colrecv[e, 1], 127, 1)
        )

    def fixed(w, m, a, r0, l0):
        rows, cols = pl.ds(r0, 8), pl.ds(l0, 128)
        k = 4 * m + a
        ends = colfix[rows, :]
        ends = pltpu.roll(ends, (-2 * k) % 128, 1) if k else ends
        at = lane + l0
        value = w[m, a, rows, cols] + jnp.where((at == 0) | (at == 255), ends, 0.0)
        if a == 0:
            value = value + jnp.where(subl + r0 == 0, rowfix[0, m : m + 1, cols], 0.0)
        if a == 3:
            value = value + jnp.where(subl + r0 == 23, rowfix[1, m : m + 1, cols], 0.0)
        return value

    def total4(values):
        return (values[0] + values[1]) + (values[2] + values[3])

    def step(k, w_in, w_out, y_old, y_new, t):
        r0, l0 = block(t)
        rows, cols = pl.ds(r0, 8), pl.ds(l0, 128)
        if k == 0:
            mass_diag = [fixed(w_in, n_modes, a, r0, l0) for a in range(4)]
            lap_diag = [fixed(w_in, n_modes + 1, a, r0, l0) for a in range(4)]
        cxs = [cx[e, rows, cols] for e in range(6)]
        for m in range(n_modes):
            scale = scale_ref[m]
            vec, rhs, old = [], [], []
            for a in range(4):
                value = fixed(w_in, m, a, r0, l0)
                w_in[m, a, rows, cols] = value
                rhs.append(value)
                if k == 0:
                    inv = 1.0 / (mass_diag[a] + scale * lap_diag[a])
                    minv[m, a, rows, cols] = inv
                    vec.append(value * inv)
                else:
                    old.append(y_old[m, a, rows, cols])
                    vec.append(value * minv[m, a, rows, cols] - old[a])
                y_new[m, a, rows, cols] = vec[a]
            lap = [None] * 4
            for e, (i, j) in enumerate(EDGES):
                flow = cxs[e] * (vec[j] - vec[i])
                lap[i] = flow if lap[i] is None else lap[i] + flow
                lap[j] = -flow if lap[j] is None else lap[j] - flow
            image = []
            for a in range(4):
                v, total = vec[a], lap[a]
                for d in (1, 2, 3):
                    flow = cy[d - 1, a, rows, cols] * (pltpu.roll(v, 128 - d, 1) - v)
                    total = total + flow - pltpu.roll(flow, d, 1)
                h = mass[a, rows, cols] * v + scale * total
                w_out[m, a, rows, cols] = h
                image.append(h)
            if k == 0:
                prod = [u * v for u, v in zip(vec, rhs)]
                part = (0.5 * (prod[0] + prod[3]) + (prod[1] + prod[2])) * col_count
                dots[0, m] += part
                dots[1, m] += total4([u * v for u, v in zip(vec, image)])
            else:
                dots[2 * k, m] += total4([u * v for u, v in zip(old, image)])
                dots[2 * k + 1, m] += total4([u * v for u, v in zip(vec, image)])

    def run_step(*args):
        def body(t, carry):
            step(*args, t)
            return carry

        lax.fori_loop(0, 6, body, 0)

    sent0 = exchange(0, w0, n_modes + 2)
    arrive(0, sent0)
    run_step(0, w0, w1, None, y0)
    sent1 = exchange(1, w1, n_modes)
    arrive(1, sent1)
    run_step(1, w1, w2, y0, y1)
    sent2 = exchange(2, w2, n_modes)
    arrive(2, sent2)
    run_step(2, w2, w3, y1, y2)

    local = jnp.zeros((8, 128), F32)
    for m in range(n_modes):
        stacked = jnp.zeros((8, 128), F32)
        for q in range(6):
            stacked = jnp.where(subl == q, jnp.sum(dots[q, m], axis=0, keepdims=True), stacked)
        local = jnp.where(lane == m, jnp.sum(stacked, axis=1, keepdims=True), local)

    def phase_sum(p, value, size, pos, member):
        red[p, pos] = value
        moves = [
            pltpu.make_async_remote_copy(
                src_ref=red.at[p, pos],
                dst_ref=red.at[p, pos],
                send_sem=rs_send.at[p, d - 1],
                recv_sem=rs_recv.at[p, d - 1],
                device_id=member(d),
                device_id_type=MESH,
            )
            for d in range(1, size)
        ]
        for move in moves:
            move.start()
        return moves

    def phase_end(p, size, moves):
        for move in moves:
            move.wait_recv()
        parts = [red[p, i] for i in range(size)]
        while len(parts) > 1:
            parts = [
                parts[i] + parts[i + 1] if i + 1 < len(parts) else parts[i]
                for i in range(0, len(parts), 2)
            ]
        return parts[0]

    moves_a = phase_sum(0, local, n_zc, zc_pos, a_member)
    sent3 = exchange(3, w3, n_modes)
    moves_b = phase_sum(1, phase_end(0, n_zc, moves_a), b_size, b_pos, b_member)
    arrive(3, sent3)
    g = phase_end(1, b_size, moves_b)

    b0, k00, k01, k11, k12, k22 = (g[q : q + 1, :] for q in range(6))
    k02 = k11
    b1 = k00 - b0
    b2 = k01 - b1
    l10 = k01 / k00
    l20 = k02 / k00
    d1 = k11 - l10 * k01
    e12 = k12 - l10 * k02
    l21 = e12 / d1
    d2 = k22 - l20 * k02 - l21 * e12
    c1 = b1 - l10 * b0
    c2 = b2 - l20 * b0 - l21 * c1
    a2 = c2 / d2
    a1 = c1 / d1 - l21 * a2
    a0 = b0 / k00 - l10 * a1 - l20 * a2
    coef = [
        [jnp.broadcast_to(v[:, m : m + 1], (8, 128)) for v in (a0, a1, a2)] for m in range(n_modes)
    ]

    def finish(t, carry):
        r0, l0 = block(t)
        rows, cols = pl.ds(r0, 8), pl.ds(l0, 128)
        for m in range(n_modes):
            u0, u1, u2 = coef[m]
            for a in range(4):
                x_ref[m, l0 // 128, natural(r0, a), :] = (
                    u0 * y0[m, a, rows, cols] + u1 * y1[m, a, rows, cols] + u2 * y2[m, a, rows, cols]
                )
                r_ref[m, l0 // 128, natural(r0, a), :] = (
                    w0[m, a, rows, cols]
                    - u0 * w1[m, a, rows, cols]
                    - u1 * w2[m, a, rows, cols]
                    - u2 * fixed(w3, m, a, r0, l0)
                )
        return carry

    lax.fori_loop(0, 6, finish, 0)
    for group in (sent0, sent1, sent2, sent3, moves_a, moves_b):
        for copy in group:
            copy.wait_send()


def solution(mesh, n_zc=None):
    n_curve, n_sub = mesh.shape["curve"], mesh.shape["sub"]
    n_zc = n_zc or 16
    n_y = n_curve // n_zc

    def step(forcing, metric, jacobian, mode_scale):
        n_modes, n_rows, n_cols = forcing.shape
        vec = pltpu.VMEM((n_modes, 4, 24, 256), F32)
        dma = pltpu.SemaphoreType.DMA
        cfg = (n_modes, n_curve, n_sub, n_zc)
        out = jax.ShapeDtypeStruct((n_modes, 2, n_rows, 128), F32)
        outs = pl.pallas_call(
            functools.partial(kernel, cfg),
            out_shape=(out, out),
            in_specs=[pl.BlockSpec(memory_space=pltpu.SMEM)]
            + [pl.BlockSpec(memory_space=pltpu.HBM)] * 3,
            out_specs=(pl.BlockSpec(memory_space=pltpu.VMEM),) * 2,
            scratch_shapes=[
                pltpu.VMEM((n_modes, 2, n_rows, 128), F32),
                pltpu.VMEM((2, n_rows, 128), F32),
                pltpu.VMEM((2, n_rows, 128), F32),
                pltpu.VMEM((n_modes + 2, 4, 24, 256), F32),
                vec, vec, vec, vec, vec, vec, vec,
                pltpu.VMEM((4, 24, 256), F32),
                pltpu.VMEM((6, 24, 256), F32),
                pltpu.VMEM((3, 4, 24, 256), F32),
                pltpu.VMEM((6, n_modes, 8, 128), F32),
                pltpu.VMEM((4, 2, 16, 256), F32),
                pltpu.VMEM((4, 24, 128), F32),
                pltpu.VMEM((4, 2, 16, 256), F32),
                pltpu.VMEM((4, 4, 16, 128), F32),
                pltpu.VMEM((4, 2, 24, 128), F32),
                pltpu.VMEM((2, 16, 256), F32),
                pltpu.VMEM((24, 128), F32),
                pltpu.VMEM((2, max(n_zc, n_y * n_sub), 8, 128), F32),
                dma((2 + n_modes, 2)),
                dma((4, 8)),
                dma((4, 8)),
                dma((2, max(n_zc, n_y * n_sub))),
                dma((2, max(n_zc, n_y * n_sub))),
            ],
            compiler_params=pltpu.CompilerParams(
                collective_id=0, has_side_effects=True, vmem_limit_bytes=40 * 1024 * 1024
            ),
        )(mode_scale, forcing, metric, jacobian)
        return tuple(jnp.swapaxes(o, 1, 2).reshape(forcing.shape) for o in outs)

    return jax.shard_map(
        step,
        mesh=mesh,
        in_specs=(P(None, "curve", "sub"), P("curve", "sub"), P("curve", "sub"), P()),
        out_specs=(P(None, "curve", "sub"), P(None, "curve", "sub")),
        check_vma=False,
    )
```

```python
import functools
import math

import jax
import jax.numpy as jnp
import numpy as np
from jax import lax
from jax.experimental import pallas as pl
from jax.experimental.pallas import tpu as pltpu
from jax.sharding import PartitionSpec as P

MESH = pl.DeviceIdType.MESH
EDGES = ((0, 1), (0, 2), (0, 3), (1, 2), (1, 3), (2, 3))
F32 = jnp.float32
VMEM_LIMIT = 61 * 1024 * 1024


def gll_slopes():
    points = np.array([-1.0, -1.0 / math.sqrt(5.0), 1.0 / math.sqrt(5.0), 1.0])
    factor = np.array(
        [np.prod([points[j] - points[m] for m in range(4) if m != j]) for j in range(4)]
    )
    slopes = np.zeros((4, 4))
    for i in range(4):
        for j in range(4):
            if i != j:
                slopes[i, j] = factor[i] / (factor[j] * (points[i] - points[j]))
        slopes[i, i] = sum((1.0 / (points[i] - points[m]) for m in range(4) if m != i))
    return slopes


def kernel(
    cfg,
    scale_ref,
    f_hbm,
    met_hbm,
    jac_hbm,
    x_ref,
    r_ref,
    fbuf,
    metbuf,
    jacbuf,
    w0,
    w1,
    w2,
    w3,
    y0,
    y1,
    y2,
    minv,
    nat,
    mass,
    cx,
    cy,
    perm,
    dots,
    rowbuf,
    cornbuf,
    colbuf,
    rowrecv,
    cornrecv,
    colrecv,
    rowfix,
    colfix,
    red,
    in_sems,
    send_sems,
    recv_sems,
    rs_send,
    rs_recv,
):
    n_modes, n_curve, n_sub, n_zc = cfg
    n_pairs = n_modes // 2
    n_y = n_curve // n_zc
    c = lax.axis_index("curve")
    s = lax.axis_index("sub")
    c_prev, c_next = lax.rem(c + n_curve - 1, n_curve), lax.rem(c + 1, n_curve)
    s_prev, s_next = lax.rem(s + n_sub - 1, n_sub), lax.rem(s + 1, n_sub)
    y_pos, zc_pos = c // n_zc, lax.rem(c, n_zc)
    b_size = n_y * n_sub
    b_pos = y_pos * n_sub + s

    halves = (pl.ds(0, 128), pl.ds(128, 128))
    loads = []
    for h in range(2):
        loads.append(pltpu.make_async_copy(met_hbm.at[:, halves[h]], metbuf.at[h], in_sems.at[0, h]))
        loads.append(pltpu.make_async_copy(jac_hbm.at[:, halves[h]], jacbuf.at[h], in_sems.at[1, h]))
    for m in range(n_modes):
        for h in range(2):
            loads.append(
                pltpu.make_async_copy(f_hbm.at[m, :, halves[h]], fbuf.at[m, h], in_sems.at[2 + m, h])
            )
    for load in loads:
        load.start()

    def a_member(d):
        pos = lax.rem(zc_pos + d, n_zc)
        return (y_pos * n_zc + pos, s)

    def b_member(d):
        pos = lax.rem(b_pos + d, b_size)
        return ((pos // n_sub) * n_zc + zc_pos, lax.rem(pos, n_sub))

    around = [
        (c_prev, s), (c_next, s), (c, s_prev), (c, s_next),
        (c_prev, s_prev), (c_prev, s_next), (c_next, s_prev), (c_next, s_next),
    ]
    partners = around + [a_member(d) for d in range(1, n_zc)] + [b_member(d) for d in range(1, b_size)]
    barrier = pltpu.get_barrier_semaphore()
    for device in partners:
        pl.semaphore_signal(barrier, inc=1, device_id=device, device_id_type=MESH)

    def lanes_of(rows):
        return lax.broadcasted_iota(jnp.int32, (rows, 128), 1)

    def rows_of(rows):
        return lax.broadcasted_iota(jnp.int32, (rows, 128), 0)

    lane, subl = lanes_of(8), rows_of(8)
    at_low, at_high, low_half = (lane & 63) == 0, (lane & 63) == 63, lane < 64
    slopes = gll_slopes()
    weights = (1.0 / 6.0, 5.0 / 6.0, 5.0 / 6.0, 1.0 / 6.0)

    big_r = lax.broadcasted_iota(jnp.int32, (256, 256), 0)
    big_c = lax.broadcasted_iota(jnp.int32, (256, 256), 1)
    for odd in range(2):
        into = ((big_r & 3) ^ odd) * 64 + (big_r >> 2) == big_c
        back = ((big_c & 3) ^ odd) * 64 + (big_c >> 2) == big_r
        perm[odd] = jnp.where(into, 1.0, 0.0).astype(jnp.bfloat16)
        perm[2 + odd] = jnp.where(back, 1.0, 0.0).astype(jnp.bfloat16)

    def select_exact(x, which):
        high = x.astype(jnp.bfloat16)
        rest = x - high.astype(F32)
        mid = rest.astype(jnp.bfloat16)
        low = (rest - mid.astype(F32)).astype(jnp.bfloat16)
        matrix = perm[which]

        def dot(part):
            return jnp.dot(part, matrix, preferred_element_type=F32)

        return (dot(high) + dot(mid)) + dot(low)

    def natural(buf):
        return jnp.concatenate(
            [
                jnp.concatenate([buf[h, pl.ds(a, 24, stride=4), :] for a in range(4)], axis=0)
                for h in range(2)
            ],
            axis=1,
        )

    def deinterleave(x_even, x_odd):
        lo = lanes_of(96) < 64
        even, odd = select_exact(x_even, 0), select_exact(x_odd, 1)
        out = []
        for q in range(2):
            e, o = even[:, 128 * q : 128 * (q + 1)], odd[:, 128 * q : 128 * (q + 1)]
            out.append(jnp.where(lo, e, o))
            out.append(pltpu.roll(jnp.where(lo, o, e), 64, 1))
        return out

    def to_natural(slot, planes, p):
        lo = lanes_of(96) < 64
        full = [jnp.concatenate([planes[p, a, b] for a in range(4)], axis=0) for b in range(4)]
        odd1, odd3 = pltpu.roll(full[1], 64, 1), pltpu.roll(full[3], 64, 1)
        even = jnp.concatenate([jnp.where(lo, full[0], odd1), jnp.where(lo, full[2], odd3)], axis=1)
        odd = jnp.concatenate([jnp.where(lo, odd1, full[0]), jnp.where(lo, odd3, full[2])], axis=1)
        for par, packed in enumerate((even, odd)):
            out = select_exact(packed, 2 + par)
            for h in range(2):
                nat[slot, 2 * p + par, h] = out[:, 128 * h : 128 * (h + 1)]

    for load in loads[:4]:
        load.wait()
    for target, buf in ((mass, jacbuf), (minv, metbuf)):
        x = natural(buf)
        for b, plane in enumerate(deinterleave(x, x)):
            for a in range(4):
                grid_w = F32(weights[a]) * F32(weights[b])
                value = plane[24 * a : 24 * (a + 1)] * grid_w
                if target is mass:
                    mass[a, b] = value
                else:
                    minv[0, a, b] = value

    def setup(t, carry):
        rows = pl.ds(pl.multiple_of(t * 8, 8), 8)
        flux = [[minv[0, a, b, rows, :] for b in range(4)] for a in range(4)]

        def mix(values, table):
            total = values[0] * F32(table[0])
            for q in range(1, 4):
                total = total + values[q] * F32(table[q])
            return total

        for b in range(4):
            column = [flux[q][b] for q in range(4)]
            for e, (i, j) in enumerate(EDGES):
                table = slopes[:, i] * slopes[:, j]
                cx[e, b, rows, :] = mix(column, table)
                cy[e, b, rows, :] = mix(flux[b], table)
            for a in range(4):
                lap = mix(column, slopes[:, a] ** 2) + mix(flux[a], slopes[:, b] ** 2)
                w0[n_pairs, a, b, rows, :] = jnp.where(low_half, mass[a, b, rows, :], lap)
        return carry

    lax.fori_loop(0, 3, setup, 0)
    dots[...] = jnp.zeros_like(dots)
    rowbuf[...] = jnp.zeros_like(rowbuf)
    cornbuf[...] = jnp.zeros_like(cornbuf)

    for p in range(n_pairs):
        for load in loads[4 + 4 * p : 8 + 4 * p]:
            load.wait()
        planes = deinterleave(natural(fbuf.at[2 * p]), natural(fbuf.at[2 * p + 1]))
        for b in range(4):
            for a in range(4):
                w0[p, a, b] = planes[b][24 * a : 24 * (a + 1)] * mass[a, b]

    lane24, row24 = lanes_of(24), rows_of(24)
    pack_key = ((lane24 + 1) & 63) >> 1

    def row_join_and_pack(e, w, pairs):
        packed = jnp.zeros((24, 128), F32)
        for p in range(pairs):
            ends = [None] * 4
            tops, bottoms = [], []
            for b in range(4):
                top, bottom = w[p, 0, b], w[p, 3, b]
                bottom = bottom + jnp.where(row24 < 23, pltpu.roll(top, 23, 0), 0.0)
                top = jnp.where(row24 > 0, pltpu.roll(bottom, 1, 0), top)
                w[p, 0, b] = top
                w[p, 3, b] = bottom
                r = 4 * p + b
                rowbuf[e, 0, r : r + 1, :] = top[0:1, :]
                rowbuf[e, 1, r : r + 1, :] = bottom[23:24, :]
                tops.append(top)
                bottoms.append(bottom)
            low_end = lane24 & 63 == 0
            corner_end = low_end[0:1]
            cornbuf[e, 0, p : p + 1, :] = jnp.where(corner_end, tops[0][0:1], tops[3][0:1])
            cornbuf[e, 1, p : p + 1, :] = jnp.where(corner_end, bottoms[0][23:24], bottoms[3][23:24])
            first = (tops[0], w[p, 1, 0], w[p, 2, 0], bottoms[0])
            last = (tops[3], w[p, 1, 3], w[p, 2, 3], bottoms[3])
            for a in range(4):
                k = 4 * p + a
                ends = jnp.where(low_end, first[a], last[a])
                ends = pltpu.roll(ends, 2 * k, 1) if k else ends
                packed = jnp.where(pack_key == k, ends, packed)
        colbuf[e] = packed

    def copies(e, pairs):
        part = pl.ds(0, -(-4 * pairs // 8) * 8)
        plan = [
            (rowbuf.at[e, 1, part], rowrecv.at[e, 0, part], (c_next, s)),
            (rowbuf.at[e, 0, part], rowrecv.at[e, 1, part], (c_prev, s)),
            (colbuf.at[e], colrecv.at[e, 0], (c, s_next)),
            (colbuf.at[e], colrecv.at[e, 1], (c, s_prev)),
            (cornbuf.at[e, 1], cornrecv.at[e, 0], (c_next, s_next)),
            (cornbuf.at[e, 1], cornrecv.at[e, 1], (c_next, s_prev)),
            (cornbuf.at[e, 0], cornrecv.at[e, 2], (c_prev, s_next)),
            (cornbuf.at[e, 0], cornrecv.at[e, 3], (c_prev, s_prev)),
        ]
        return [
            pltpu.make_async_remote_copy(
                src_ref=src,
                dst_ref=dst,
                send_sem=send_sems.at[e, i],
                recv_sem=recv_sems.at[e, i],
                device_id=device,
                device_id_type=MESH,
            )
            for i, (src, dst, device) in reversed(list(enumerate(plan)))
        ]

    def exchange(e, w, pairs):
        row_join_and_pack(e, w, pairs)
        if e == 0:
            pl.semaphore_wait(barrier, len(partners))
        sent = copies(e, pairs)
        for copy in sent:
            copy.start()
        inner_high, inner_low = lane24 & 63 != 63, lane24 & 63 != 0
        for p in range(pairs):
            for a in range(4):
                first, last = w[p, a, 0], w[p, a, 3]
                last = last + jnp.where(inner_high, pltpu.roll(first, 127, 1), 0.0)
                w[p, a, 3] = last
                w[p, a, 0] = jnp.where(inner_low, pltpu.roll(last, 1, 1), first)
        return sent

    def arrive(e, sent, pairs):
        for copy in sent:
            copy.wait_recv()
        count = -(-4 * pairs // 8) * 8
        lanes, rows = lanes_of(count) & 63, rows_of(count) & 3
        for side in range(2):
            r = rowrecv[e, side, 0:count, :]
            t = pltpu.roll(pltpu.roll(r, 127, 1), 3, 0)
            u = r + jnp.where((rows == 3) & (lanes != 63), t, 0.0)
            v = pltpu.roll(pltpu.roll(u, 1, 1), count - 3, 0)
            rowfix[side, 0:count, :] = jnp.where((rows == 0) & (lanes != 0), v, u)
            left = pltpu.roll(cornrecv[e, 2 * side], 65, 1)
            right = pltpu.roll(cornrecv[e, 2 * side + 1], 63, 1)
            left = jnp.where(at_low, left, 0.0)
            right = jnp.where(at_high, right, 0.0)
            for p in range(pairs):
                rowfix[side, 4 * p : 4 * p + 1, :] += left[p : p + 1]
                rowfix[side, 4 * p + 3 : 4 * p + 4, :] += right[p : p + 1]
        colfix[...] = jnp.where(
            (lane24 & 1) == 0, pltpu.roll(colrecv[e, 0], 65, 1), pltpu.roll(colrecv[e, 1], 63, 1)
        )

    def fixed(w, p, r0):
        rows = pl.ds(r0, 8)
        out = []
        for a in range(4):
            k = 4 * p + a
            ends = colfix[rows, :]
            ends = pltpu.roll(ends, (-2 * k) % 128, 1) if k else ends
            line = []
            for b in range(4):
                value = w[p, a, b, rows, :]
                if b == 0:
                    value = value + jnp.where(at_low, ends, 0.0)
                if b == 3:
                    value = value + jnp.where(at_high, ends, 0.0)
                r = 4 * p + b
                if a == 0:
                    value = value + jnp.where(subl + r0 == 0, rowfix[0, r : r + 1, :], 0.0)
                if a == 3:
                    value = value + jnp.where(subl + r0 == 23, rowfix[1, r : r + 1, :], 0.0)
                line.append(value)
            out.append(line)
        return out

    def total(values):
        values = list(values)
        while len(values) > 1:
            values = [
                values[i] + values[i + 1] if i + 1 < len(values) else values[i]
                for i in range(0, len(values), 2)
            ]
        return values[0]

    quad = [(a, b) for a in range(4) for b in range(4)]

    def step(k, w_in, w_out, y_old, y_new, t):
        r0 = pl.multiple_of(t * 8, 8)
        rows = pl.ds(r0, 8)
        if k == 0:
            both = fixed(w_in, n_pairs, r0)
            for a, b in quad:
                swapped = pltpu.roll(both[a][b], 64, 1)
                w_in[n_pairs, a, b, rows, :] = jnp.where(low_half, both[a][b], swapped)
                y2[0, a, b, rows, :] = jnp.where(low_half, swapped, both[a][b])
        for p in range(n_pairs):
            scale = jnp.where(low_half, scale_ref[2 * p], scale_ref[2 * p + 1])
            value = fixed(w_in, p, r0)
            vec = [[None] * 4 for _ in range(4)]
            for a, b in quad:
                w_in[p, a, b, rows, :] = value[a][b]
                if k == 0:
                    diag = w_in[n_pairs, a, b, rows, :] + scale * y2[0, a, b, rows, :]
                    inv = 1.0 / diag
                    minv[p, a, b, rows, :] = inv
                    vec[a][b] = value[a][b] * inv
                else:
                    vec[a][b] = value[a][b] * minv[p, a, b, rows, :] - y_old[p, a, b, rows, :]
                y_new[p, a, b, rows, :] = vec[a][b]
            lap = [[None] * 4 for _ in range(4)]

            def flow(table, e, line, i, j):
                (ai, bi), (aj, bj) = i, j
                f = table[e, line, rows, :] * (vec[aj][bj] - vec[ai][bi])
                lap[ai][bi] = f if lap[ai][bi] is None else lap[ai][bi] + f
                lap[aj][bj] = -f if lap[aj][bj] is None else lap[aj][bj] - f

            for line in range(4):
                for e, (i, j) in enumerate(EDGES):
                    flow(cx, e, line, (i, line), (j, line))
            image = [[None] * 4 for _ in range(4)]
            for a in range(4):
                for e, (i, j) in enumerate(EDGES):
                    flow(cy, e, a, (a, i), (a, j))
                for b in range(4):
                    image[a][b] = mass[a, b, rows, :] * vec[a][b] + scale * lap[a][b]
                    w_out[p, a, b, rows, :] = image[a][b]
            if k == 0:
                count = (0.5, 1.0, 1.0, 0.5)
                terms = []
                for a, b in quad:
                    term = vec[a][b] * value[a][b]
                    weight = count[a] * count[b]
                    terms.append(term if weight == 1.0 else term * F32(weight))
                dots[0, p] += total(terms)
                dots[1, p] += total(vec[a][b] * image[a][b] for a, b in quad)
            else:
                dots[2 * k, p] += total(y_old[p, a, b, rows, :] * image[a][b] for a, b in quad)
                dots[2 * k + 1, p] += total(vec[a][b] * image[a][b] for a, b in quad)

    def run_step(*args):
        def body(t, carry):
            step(*args, t)
            return carry

        lax.fori_loop(0, 3, body, 0)

    sent0 = exchange(0, w0, n_pairs + 1)
    arrive(0, sent0, n_pairs + 1)
    run_step(0, w0, w1, None, y0)
    sent1 = exchange(1, w1, n_pairs)
    arrive(1, sent1, n_pairs)
    run_step(1, w1, w2, y0, y1)
    sent2 = exchange(2, w2, n_pairs)
    arrive(2, sent2, n_pairs)
    run_step(2, w2, w3, y1, y2)

    local = jnp.zeros((8, 128), F32)
    for p in range(n_pairs):
        stacked = jnp.zeros((8, 128), F32)
        for q in range(6):
            stacked = jnp.where(subl == q, jnp.sum(dots[q, p], axis=0, keepdims=True), stacked)
        for par in range(2):
            half = jnp.where(low_half, stacked, 0.0) if par == 0 else jnp.where(low_half, 0.0, stacked)
            local = jnp.where(lane == 2 * p + par, jnp.sum(half, axis=1, keepdims=True), local)

    def phase_start(i, value, size, pos, member):
        red[i, pos] = value
        moves = [
            pltpu.make_async_remote_copy(
                src_ref=red.at[i, pos],
                dst_ref=red.at[i, pos],
                send_sem=rs_send.at[i, d - 1],
                recv_sem=rs_recv.at[i, d - 1],
                device_id=member(d),
                device_id_type=MESH,
            )
            for d in range(1, size)
        ]
        for move in moves:
            move.start()
        return moves

    def phase_end(i, size, moves):
        for move in moves:
            move.wait_recv()
        return total(red[i, j] for j in range(size))

    def run_natural(slot, planes):
        for p in range(n_pairs):
            to_natural(slot, planes, p)

    moves_a = phase_start(0, local, n_zc, zc_pos, a_member)
    sent3 = exchange(3, w3, n_pairs)
    for slot, planes in enumerate((y0, y1, y2)):
        run_natural(slot, planes)
    moves_b = phase_start(1, phase_end(0, n_zc, moves_a), b_size, b_pos, b_member)
    for slot, planes in enumerate((w0, w1, w2)):
        run_natural(3 + slot, planes)
    arrive(3, sent3, n_pairs)

    def last_fix(t, carry):
        r0 = pl.multiple_of(t * 8, 8)
        for p in range(n_pairs):
            value = fixed(w3, p, r0)
            for a, b in quad:
                w3[p, a, b, pl.ds(r0, 8), :] = value[a][b]
        return carry

    lax.fori_loop(0, 3, last_fix, 0)
    run_natural(6, w3)
    g = phase_end(1, b_size, moves_b)

    b0, k00, k01, k11, k12, k22 = (g[q : q + 1, :] for q in range(6))
    k02 = k11
    b1 = k00 - b0
    b2 = k01 - b1
    l10 = k01 / k00
    l20 = k02 / k00
    d1 = k11 - l10 * k01
    e12 = k12 - l10 * k02
    l21 = e12 / d1
    d2 = k22 - l20 * k02 - l21 * e12
    c1 = b1 - l10 * b0
    c2 = b2 - l20 * b0 - l21 * c1
    a2 = c2 / d2
    a1 = c1 / d1 - l21 * a2
    a0 = b0 / k00 - l10 * a1 - l20 * a2

    for m in range(n_modes):
        u0, u1, u2 = (jnp.broadcast_to(v[:, m : m + 1], (8, 128)) for v in (a0, a1, a2))
        for h in range(2):
            for a in range(4):
                for t in range(3):
                    src = pl.ds(24 * a + 8 * t, 8)
                    dst = pl.ds(a + 32 * t, 8, stride=4)
                    n = [nat[i, m, h, src, :] for i in range(7)]
                    x_ref[m, h, dst, :] = u0 * n[0] + u1 * n[1] + u2 * n[2]
                    r_ref[m, h, dst, :] = n[3] - u0 * n[4] - u1 * n[5] - u2 * n[6]
    for group in (sent0, sent1, sent2, sent3, moves_a, moves_b):
        for copy in group:
            copy.wait_send()


def solution(mesh, n_zc=None):
    n_curve, n_sub = mesh.shape["curve"], mesh.shape["sub"]
    n_zc = n_zc or 16
    n_y = n_curve // n_zc

    def step(forcing, metric, jacobian, mode_scale):
        n_modes, n_rows, n_cols = forcing.shape
        n_pairs = n_modes // 2
        vec = pltpu.VMEM((n_pairs, 4, 4, 24, 128), F32)
        dma = pltpu.SemaphoreType.DMA
        cfg = (n_modes, n_curve, n_sub, n_zc)
        out = jax.ShapeDtypeStruct((n_modes, 2, n_rows, 128), F32)
        slots = max(n_zc, n_y * n_sub)
        outs = pl.pallas_call(
            functools.partial(kernel, cfg),
            out_shape=(out, out),
            in_specs=[pl.BlockSpec(memory_space=pltpu.SMEM)]
            + [pl.BlockSpec(memory_space=pltpu.HBM)] * 3,
            out_specs=(pl.BlockSpec(memory_space=pltpu.VMEM),) * 2,
            scratch_shapes=[
                pltpu.VMEM((n_modes, 2, n_rows, 128), F32),
                pltpu.VMEM((2, n_rows, 128), F32),
                pltpu.VMEM((2, n_rows, 128), F32),
                pltpu.VMEM((n_pairs + 1, 4, 4, 24, 128), F32),
                vec, vec, vec, vec, vec, vec, vec,
                pltpu.VMEM((7, n_modes, 2, n_rows, 128), F32),
                pltpu.VMEM((4, 4, 24, 128), F32),
                pltpu.VMEM((6, 4, 24, 128), F32),
                pltpu.VMEM((6, 4, 24, 128), F32),
                pltpu.VMEM((4, 256, 256), jnp.bfloat16),
                pltpu.VMEM((6, n_pairs, 8, 128), F32),
                pltpu.VMEM((4, 2, 32, 128), F32),
                pltpu.VMEM((4, 2, 8, 128), F32),
                pltpu.VMEM((4, 24, 128), F32),
                pltpu.VMEM((4, 2, 32, 128), F32),
                pltpu.VMEM((4, 4, 8, 128), F32),
                pltpu.VMEM((4, 2, 24, 128), F32),
                pltpu.VMEM((2, 32, 128), F32),
                pltpu.VMEM((24, 128), F32),
                pltpu.VMEM((2, slots, 8, 128), F32),
                dma((2 + n_modes, 2)),
                dma((4, 8)),
                dma((4, 8)),
                dma((2, slots)),
                dma((2, slots)),
            ],
            compiler_params=pltpu.CompilerParams(
                collective_id=0, has_side_effects=True, vmem_limit_bytes=VMEM_LIMIT
            ),
        )(mode_scale, forcing, metric, jacobian)
        return tuple(jnp.swapaxes(o, 1, 2).reshape(forcing.shape) for o in outs)

    return jax.shard_map(
        step,
        mesh=mesh,
        in_specs=(P(None, "curve", "sub"), P("curve", "sub"), P("curve", "sub"), P()),
        out_specs=(P(None, "curve", "sub"), P(None, "curve", "sub")),
        check_vma=False,
    )
```

```python
import functools
import math

import jax
import jax.numpy as jnp
import numpy as np
from jax import lax
from jax.experimental import pallas as pl
from jax.experimental.pallas import tpu as pltpu
from jax.sharding import PartitionSpec as P

MESH = pl.DeviceIdType.MESH
EDGES = ((0, 1), (0, 2), (0, 3), (1, 2), (1, 3), (2, 3))
F32 = jnp.float32
VMEM_LIMIT = 40 * 1024 * 1024


def gll_slopes():
    points = np.array([-1.0, -1.0 / math.sqrt(5.0), 1.0 / math.sqrt(5.0), 1.0])
    factor = np.array(
        [np.prod([points[j] - points[m] for m in range(4) if m != j]) for j in range(4)]
    )
    slopes = np.zeros((4, 4))
    for i in range(4):
        for j in range(4):
            if i != j:
                slopes[i, j] = factor[i] / (factor[j] * (points[i] - points[j]))
        slopes[i, i] = sum((1.0 / (points[i] - points[m]) for m in range(4) if m != i))
    return slopes


def kernel(
    cfg,
    scale_hbm,
    f_hbm,
    met_hbm,
    jac_hbm,
    x_ref,
    r_ref,
    scale_ref,
    fbuf,
    metbuf,
    jacbuf,
    w0,
    w1,
    w2,
    w3,
    y0,
    y1,
    y2,
    minv,
    nat,
    mass,
    cx,
    cy,
    perm,
    dots,
    rowbuf,
    cornbuf,
    colbuf,
    rowrecv,
    cornrecv,
    colrecv,
    rowfix,
    colfix,
    red,
    in_sems,
    send_sems,
    recv_sems,
    rs_send,
    rs_recv,
):
    n_modes, n_curve, n_sub, n_zc = cfg
    n_pairs = n_modes // 2
    n_y = n_curve // n_zc
    c = lax.axis_index("curve")
    s = lax.axis_index("sub")
    c_prev, c_next = lax.rem(c + n_curve - 1, n_curve), lax.rem(c + 1, n_curve)
    s_prev, s_next = lax.rem(s + n_sub - 1, n_sub), lax.rem(s + 1, n_sub)
    y_pos, zc_pos = c // n_zc, lax.rem(c, n_zc)
    b_size = n_y * n_sub
    b_pos = y_pos * n_sub + s

    halves = (pl.ds(0, 128), pl.ds(128, 128))
    loads = []
    for h in range(2):
        loads.append(pltpu.make_async_copy(met_hbm.at[:, halves[h]], metbuf.at[h], in_sems.at[0, h]))
        loads.append(pltpu.make_async_copy(jac_hbm.at[:, halves[h]], jacbuf.at[h], in_sems.at[1, h]))
    for m in range(n_modes):
        for h in range(2):
            loads.append(
                pltpu.make_async_copy(f_hbm.at[m, :, halves[h]], fbuf.at[m, h], in_sems.at[2 + m, h])
            )
    loads.append(pltpu.make_async_copy(scale_hbm, scale_ref, in_sems.at[2 + n_modes, 0]))
    for load in loads:
        load.start()

    def a_member(d):
        pos = lax.rem(zc_pos + d, n_zc)
        return (y_pos * n_zc + pos, s)

    def b_member(d):
        pos = lax.rem(b_pos + d, b_size)
        return ((pos // n_sub) * n_zc + zc_pos, lax.rem(pos, n_sub))

    around = [
        (c_prev, s), (c_next, s), (c, s_prev), (c, s_next),
        (c_prev, s_prev), (c_prev, s_next), (c_next, s_prev), (c_next, s_next),
    ]
    partners = around + [a_member(d) for d in range(1, n_zc)] + [b_member(d) for d in range(1, b_size)]
    barrier = pltpu.get_barrier_semaphore()
    for device in partners:
        pl.semaphore_signal(barrier, inc=1, device_id=device, device_id_type=MESH)

    def lanes_of(rows):
        return lax.broadcasted_iota(jnp.int32, (rows, 128), 1)

    def rows_of(rows):
        return lax.broadcasted_iota(jnp.int32, (rows, 128), 0)

    lane, subl = lanes_of(8), rows_of(8)
    at_low, at_high, low_half = (lane & 63) == 0, (lane & 63) == 63, lane < 64
    slopes = gll_slopes()
    weights = (1.0 / 6.0, 5.0 / 6.0, 5.0 / 6.0, 1.0 / 6.0)

    big_r = lax.broadcasted_iota(jnp.int32, (256, 256), 0)
    big_c = lax.broadcasted_iota(jnp.int32, (256, 256), 1)
    for odd in range(2):
        into = ((big_r & 3) ^ odd) * 64 + (big_r >> 2) == big_c
        back = ((big_c & 3) ^ odd) * 64 + (big_c >> 2) == big_r
        perm[odd] = jnp.where(into, 1.0, 0.0).astype(jnp.bfloat16)
        perm[2 + odd] = jnp.where(back, 1.0, 0.0).astype(jnp.bfloat16)

    def select_exact(x, which):
        high = x.astype(jnp.bfloat16)
        rest = x - high.astype(F32)
        mid = rest.astype(jnp.bfloat16)
        low = (rest - mid.astype(F32)).astype(jnp.bfloat16)
        matrix = perm[which]

        def dot(part):
            return jnp.dot(part, matrix, preferred_element_type=F32)

        return (dot(high) + dot(mid)) + dot(low)

    def natural(buf):
        return jnp.concatenate(
            [
                jnp.concatenate([buf[h, pl.ds(a, 24, stride=4), :] for a in range(4)], axis=0)
                for h in range(2)
            ],
            axis=1,
        )

    def deinterleave(x_even, x_odd):
        lo = lanes_of(96) < 64
        even, odd = select_exact(x_even, 0), select_exact(x_odd, 1)
        out = []
        for q in range(2):
            e, o = even[:, 128 * q : 128 * (q + 1)], odd[:, 128 * q : 128 * (q + 1)]
            out.append(jnp.where(lo, e, o))
            out.append(pltpu.roll(jnp.where(lo, o, e), 64, 1))
        return out

    def to_natural(slot, planes, p):
        lo = lanes_of(96) < 64
        full = [jnp.concatenate([planes[p, a, b] for a in range(4)], axis=0) for b in range(4)]
        odd1, odd3 = pltpu.roll(full[1], 64, 1), pltpu.roll(full[3], 64, 1)
        even = jnp.concatenate([jnp.where(lo, full[0], odd1), jnp.where(lo, full[2], odd3)], axis=1)
        odd = jnp.concatenate([jnp.where(lo, odd1, full[0]), jnp.where(lo, odd3, full[2])], axis=1)
        for par, packed in enumerate((even, odd)):
            out = select_exact(packed, 2 + par)
            for h in range(2):
                nat[slot, 2 * p + par, h] = out[:, 128 * h : 128 * (h + 1)]

    for load in loads[:4]:
        load.wait()
    for target, buf in ((mass, jacbuf), (minv, metbuf)):
        x = natural(buf)
        for b, plane in enumerate(deinterleave(x, x)):
            for a in range(4):
                grid_w = F32(weights[a]) * F32(weights[b])
                value = plane[24 * a : 24 * (a + 1)] * grid_w
                if target is mass:
                    mass[a, b] = value
                else:
                    minv[0, a, b] = value

    def setup(t, carry):
        rows = pl.ds(pl.multiple_of(t * 8, 8), 8)
        flux = [[minv[0, a, b, rows, :] for b in range(4)] for a in range(4)]

        def mix(values, table):
            total = values[0] * F32(table[0])
            for q in range(1, 4):
                total = total + values[q] * F32(table[q])
            return total

        for b in range(4):
            column = [flux[q][b] for q in range(4)]
            for e, (i, j) in enumerate(EDGES):
                table = slopes[:, i] * slopes[:, j]
                cx[e, b, rows, :] = mix(column, table)
                cy[e, b, rows, :] = mix(flux[b], table)
            for a in range(4):
                lap = mix(column, slopes[:, a] ** 2) + mix(flux[a], slopes[:, b] ** 2)
                w0[n_pairs, a, b, rows, :] = jnp.where(low_half, mass[a, b, rows, :], lap)
        return carry

    lax.fori_loop(0, 3, setup, 0)
    dots[...] = jnp.zeros_like(dots)
    rowbuf[...] = jnp.zeros_like(rowbuf)
    cornbuf[...] = jnp.zeros_like(cornbuf)

    for p in range(n_pairs):
        for load in loads[4 + 4 * p : 8 + 4 * p]:
            load.wait()
        planes = deinterleave(natural(fbuf.at[2 * p]), natural(fbuf.at[2 * p + 1]))
        for b in range(4):
            for a in range(4):
                w0[p, a, b] = planes[b][24 * a : 24 * (a + 1)] * mass[a, b]

    lane24, row24 = lanes_of(24), rows_of(24)
    pack_key = ((lane24 + 1) & 63) >> 1

    def row_join_and_pack(e, w, pairs):
        packed = jnp.zeros((24, 128), F32)
        for p in range(pairs):
            ends = [None] * 4
            tops, bottoms = [], []
            for b in range(4):
                top, bottom = w[p, 0, b], w[p, 3, b]
                bottom = bottom + jnp.where(row24 < 23, pltpu.roll(top, 23, 0), 0.0)
                top = jnp.where(row24 > 0, pltpu.roll(bottom, 1, 0), top)
                w[p, 0, b] = top
                w[p, 3, b] = bottom
                r = 4 * p + b
                rowbuf[e, 0, r : r + 1, :] = top[0:1, :]
                rowbuf[e, 1, r : r + 1, :] = bottom[23:24, :]
                tops.append(top)
                bottoms.append(bottom)
            low_end = lane24 & 63 == 0
            corner_end = low_end[0:1]
            cornbuf[e, 0, p : p + 1, :] = jnp.where(corner_end, tops[0][0:1], tops[3][0:1])
            cornbuf[e, 1, p : p + 1, :] = jnp.where(corner_end, bottoms[0][23:24], bottoms[3][23:24])
            first = (tops[0], w[p, 1, 0], w[p, 2, 0], bottoms[0])
            last = (tops[3], w[p, 1, 3], w[p, 2, 3], bottoms[3])
            for a in range(4):
                k = 4 * p + a
                ends = jnp.where(low_end, first[a], last[a])
                ends = pltpu.roll(ends, 2 * k, 1) if k else ends
                packed = jnp.where(pack_key == k, ends, packed)
        colbuf[e] = packed

    def copies(e, pairs):
        part = pl.ds(0, -(-4 * pairs // 8) * 8)
        plan = [
            (rowbuf.at[e, 1, part], rowrecv.at[e, 0, part], (c_next, s)),
            (rowbuf.at[e, 0, part], rowrecv.at[e, 1, part], (c_prev, s)),
            (colbuf.at[e], colrecv.at[e, 0], (c, s_next)),
            (colbuf.at[e], colrecv.at[e, 1], (c, s_prev)),
            (cornbuf.at[e, 1], cornrecv.at[e, 0], (c_next, s_next)),
            (cornbuf.at[e, 1], cornrecv.at[e, 1], (c_next, s_prev)),
            (cornbuf.at[e, 0], cornrecv.at[e, 2], (c_prev, s_next)),
            (cornbuf.at[e, 0], cornrecv.at[e, 3], (c_prev, s_prev)),
        ]
        return [
            pltpu.make_async_remote_copy(
                src_ref=src,
                dst_ref=dst,
                send_sem=send_sems.at[e, i],
                recv_sem=recv_sems.at[e, i],
                device_id=device,
                device_id_type=MESH,
            )
            for i, (src, dst, device) in enumerate(plan)
        ]

    def exchange(e, w, pairs):
        row_join_and_pack(e, w, pairs)
        if e == 0:
            pl.semaphore_wait(barrier, len(partners))
        sent = copies(e, pairs)
        for copy in reversed(sent):
            copy.start()
        inner_high, inner_low = lane24 & 63 != 63, lane24 & 63 != 0
        for p in range(pairs):
            for a in range(4):
                first, last = w[p, a, 0], w[p, a, 3]
                last = last + jnp.where(inner_high, pltpu.roll(first, 127, 1), 0.0)
                w[p, a, 3] = last
                w[p, a, 0] = jnp.where(inner_low, pltpu.roll(last, 1, 1), first)
        return sent

    def arrive_cols(e, sent):
        for copy in sent[2:4]:
            copy.wait_recv()
        colfix[...] = jnp.where(
            (lane24 & 1) == 0, pltpu.roll(colrecv[e, 0], 65, 1), pltpu.roll(colrecv[e, 1], 63, 1)
        )

    def arrive_rows(e, sent, pairs):
        for copy in sent[:2] + sent[4:]:
            copy.wait_recv()
        count = -(-4 * pairs // 8) * 8
        lanes, rows = lanes_of(count) & 63, rows_of(count) & 3
        for side in range(2):
            r = rowrecv[e, side, 0:count, :]
            t = pltpu.roll(pltpu.roll(r, 127, 1), 3, 0)
            u = r + jnp.where((rows == 3) & (lanes != 63), t, 0.0)
            v = pltpu.roll(pltpu.roll(u, 1, 1), count - 3, 0)
            rowfix[side, 0:count, :] = jnp.where((rows == 0) & (lanes != 0), v, u)
            left = pltpu.roll(cornrecv[e, 2 * side], 65, 1)
            right = pltpu.roll(cornrecv[e, 2 * side + 1], 63, 1)
            left = jnp.where(at_low, left, 0.0)
            right = jnp.where(at_high, right, 0.0)
            for p in range(pairs):
                rowfix[side, 4 * p : 4 * p + 1, :] += left[p : p + 1]
                rowfix[side, 4 * p + 3 : 4 * p + 4, :] += right[p : p + 1]

    def fixed(w, p, r0, outer):
        rows = pl.ds(r0, 8)
        out = []
        for a in range(4):
            k = 4 * p + a
            ends = colfix[rows, :]
            ends = pltpu.roll(ends, (-2 * k) % 128, 1) if k else ends
            line = []
            for b in range(4):
                value = w[p, a, b, rows, :]
                if b == 0:
                    value = value + jnp.where(at_low, ends, 0.0)
                if b == 3:
                    value = value + jnp.where(at_high, ends, 0.0)
                r = 4 * p + b
                if outer and a == 0:
                    value = value + jnp.where(subl + r0 == 0, rowfix[0, r : r + 1, :], 0.0)
                if outer and a == 3:
                    value = value + jnp.where(subl + r0 == 23, rowfix[1, r : r + 1, :], 0.0)
                line.append(value)
            out.append(line)
        return out

    def total(values):
        values = list(values)
        while len(values) > 1:
            values = [
                values[i] + values[i + 1] if i + 1 < len(values) else values[i]
                for i in range(0, len(values), 2)
            ]
        return values[0]

    quad = [(a, b) for a in range(4) for b in range(4)]

    def step(k, w_in, w_out, y_old, y_new, t, outer):
        r0 = pl.multiple_of(t * 8, 8) if outer else 8 * t
        rows = pl.ds(r0, 8)
        if k == 0:
            both = fixed(w_in, n_pairs, r0, outer)
            for a, b in quad:
                swapped = pltpu.roll(both[a][b], 64, 1)
                w_in[n_pairs, a, b, rows, :] = jnp.where(low_half, both[a][b], swapped)
                y2[0, a, b, rows, :] = jnp.where(low_half, swapped, both[a][b])
        for p in range(n_pairs):
            scale = jnp.where(low_half, scale_ref[2 * p], scale_ref[2 * p + 1])
            value = fixed(w_in, p, r0, outer)
            vec = [[None] * 4 for _ in range(4)]
            for a, b in quad:
                w_in[p, a, b, rows, :] = value[a][b]
                if k == 0:
                    diag = w_in[n_pairs, a, b, rows, :] + scale * y2[0, a, b, rows, :]
                    inv = 1.0 / diag
                    minv[p, a, b, rows, :] = inv
                    vec[a][b] = value[a][b] * inv
                else:
                    vec[a][b] = value[a][b] * minv[p, a, b, rows, :] - y_old[p, a, b, rows, :]
                y_new[p, a, b, rows, :] = vec[a][b]
            lap = [[None] * 4 for _ in range(4)]

            def flow(table, e, line, i, j):
                (ai, bi), (aj, bj) = i, j
                f = table[e, line, rows, :] * (vec[aj][bj] - vec[ai][bi])
                lap[ai][bi] = f if lap[ai][bi] is None else lap[ai][bi] + f
                lap[aj][bj] = -f if lap[aj][bj] is None else lap[aj][bj] - f

            for line in range(4):
                for e, (i, j) in enumerate(EDGES):
                    flow(cx, e, line, (i, line), (j, line))
            image = [[None] * 4 for _ in range(4)]
            for a in range(4):
                for e, (i, j) in enumerate(EDGES):
                    flow(cy, e, a, (a, i), (a, j))
                for b in range(4):
                    image[a][b] = mass[a, b, rows, :] * vec[a][b] + scale * lap[a][b]
                    w_out[p, a, b, rows, :] = image[a][b]
            if k == 0:
                count = (0.5, 1.0, 1.0, 0.5)
                terms = []
                for a, b in quad:
                    term = vec[a][b] * value[a][b]
                    weight = count[a] * count[b]
                    terms.append(term if weight == 1.0 else term * F32(weight))
                dots[0, p] += total(terms)
                dots[1, p] += total(vec[a][b] * image[a][b] for a, b in quad)
            else:
                dots[2 * k, p] += total(y_old[p, a, b, rows, :] * image[a][b] for a, b in quad)
                dots[2 * k + 1, p] += total(vec[a][b] * image[a][b] for a, b in quad)

    def run_step(e, sent, pairs, *args):
        def body(i, carry):
            step(*args, 2 * i, True)
            return carry

        arrive_cols(e, sent)
        step(*args, 1, False)
        arrive_rows(e, sent, pairs)
        lax.fori_loop(0, 2, body, 0)

    sent0 = exchange(0, w0, n_pairs + 1)
    loads[-1].wait()
    run_step(0, sent0, n_pairs + 1, 0, w0, w1, None, y0)
    sent1 = exchange(1, w1, n_pairs)
    run_step(1, sent1, n_pairs, 1, w1, w2, y0, y1)
    sent2 = exchange(2, w2, n_pairs)
    run_step(2, sent2, n_pairs, 2, w2, w3, y1, y2)

    local = jnp.zeros((8, 128), F32)
    for p in range(n_pairs):
        stacked = jnp.zeros((8, 128), F32)
        for q in range(6):
            stacked = jnp.where(subl == q, jnp.sum(dots[q, p], axis=0, keepdims=True), stacked)
        for par in range(2):
            half = jnp.where(low_half, stacked, 0.0) if par == 0 else jnp.where(low_half, 0.0, stacked)
            local = jnp.where(lane == 2 * p + par, jnp.sum(half, axis=1, keepdims=True), local)

    def phase_start(i, value, size, pos, member):
        red[i, pos] = value
        moves = [
            pltpu.make_async_remote_copy(
                src_ref=red.at[i, pos],
                dst_ref=red.at[i, pos],
                send_sem=rs_send.at[i, d - 1],
                recv_sem=rs_recv.at[i, d - 1],
                device_id=member(d),
                device_id_type=MESH,
            )
            for d in range(1, size)
        ]
        for move in moves:
            move.start()
        return moves

    def phase_end(i, size, moves):
        for move in moves:
            move.wait_recv()
        return total(red[i, j] for j in range(size))

    def run_natural(slot, planes):
        for p in range(n_pairs):
            to_natural(slot, planes, p)

    moves_a = phase_start(0, local, n_zc, zc_pos, a_member)
    sent3 = exchange(3, w3, n_pairs)
    for slot, planes in enumerate((y0, y1, y2)):
        run_natural(slot, planes)
    moves_b = phase_start(1, phase_end(0, n_zc, moves_a), b_size, b_pos, b_member)
    for slot, planes in enumerate((w0, w1, w2)):
        run_natural(3 + slot, planes)
    arrive_cols(3, sent3)
    arrive_rows(3, sent3, n_pairs)

    def last_fix(t, carry):
        r0 = pl.multiple_of(t * 8, 8)
        for p in range(n_pairs):
            value = fixed(w3, p, r0, True)
            for a, b in quad:
                w3[p, a, b, pl.ds(r0, 8), :] = value[a][b]
        return carry

    lax.fori_loop(0, 3, last_fix, 0)
    run_natural(6, w3)
    g = phase_end(1, b_size, moves_b)

    b0, k00, k01, k11, k12, k22 = (g[q : q + 1, :] for q in range(6))
    k02 = k11
    b1 = k00 - b0
    b2 = k01 - b1
    l10 = k01 / k00
    l20 = k02 / k00
    d1 = k11 - l10 * k01
    e12 = k12 - l10 * k02
    l21 = e12 / d1
    d2 = k22 - l20 * k02 - l21 * e12
    c1 = b1 - l10 * b0
    c2 = b2 - l20 * b0 - l21 * c1
    a2 = c2 / d2
    a1 = c1 / d1 - l21 * a2
    a0 = b0 / k00 - l10 * a1 - l20 * a2

    for m in range(n_modes):
        u0, u1, u2 = (jnp.broadcast_to(v[:, m : m + 1], (8, 128)) for v in (a0, a1, a2))
        for h in range(2):
            for a in range(4):
                for t in range(3):
                    src = pl.ds(24 * a + 8 * t, 8)
                    dst = pl.ds(a + 32 * t, 8, stride=4)
                    n = [nat[i, m, h, src, :] for i in range(7)]
                    x_ref[m, h, dst, :] = u0 * n[0] + u1 * n[1] + u2 * n[2]
                    r_ref[m, h, dst, :] = n[3] - u0 * n[4] - u1 * n[5] - u2 * n[6]
    for group in (sent0, sent1, sent2, sent3, moves_a, moves_b):
        for copy in group:
            copy.wait_send()


def solution(mesh, n_zc=None):
    n_curve, n_sub = mesh.shape["curve"], mesh.shape["sub"]
    n_zc = n_zc or 16
    n_y = n_curve // n_zc

    def step(forcing, metric, jacobian, mode_scale):
        n_modes, n_rows, n_cols = forcing.shape
        n_pairs = n_modes // 2
        vec = pltpu.VMEM((n_pairs, 4, 4, 24, 128), F32)
        dma = pltpu.SemaphoreType.DMA
        cfg = (n_modes, n_curve, n_sub, n_zc)
        out = jax.ShapeDtypeStruct((n_modes, 2, n_rows, 128), F32)
        slots = max(n_zc, n_y * n_sub)
        outs = pl.pallas_call(
            functools.partial(kernel, cfg),
            out_shape=(out, out),
            in_specs=[pl.BlockSpec(memory_space=pltpu.HBM)] * 4,
            out_specs=(pl.BlockSpec(memory_space=pltpu.VMEM),) * 2,
            scratch_shapes=[
                pltpu.SMEM((n_modes,), F32),
                pltpu.VMEM((n_modes, 2, n_rows, 128), F32),
                pltpu.VMEM((2, n_rows, 128), F32),
                pltpu.VMEM((2, n_rows, 128), F32),
                pltpu.VMEM((n_pairs + 1, 4, 4, 24, 128), F32),
                vec, vec, vec, vec, vec, vec, vec,
                pltpu.VMEM((7, n_modes, 2, n_rows, 128), F32),
                pltpu.VMEM((4, 4, 24, 128), F32),
                pltpu.VMEM((6, 4, 24, 128), F32),
                pltpu.VMEM((6, 4, 24, 128), F32),
                pltpu.VMEM((4, 256, 256), jnp.bfloat16),
                pltpu.VMEM((6, n_pairs, 8, 128), F32),
                pltpu.VMEM((4, 2, 32, 128), F32),
                pltpu.VMEM((4, 2, 8, 128), F32),
                pltpu.VMEM((4, 24, 128), F32),
                pltpu.VMEM((4, 2, 32, 128), F32),
                pltpu.VMEM((4, 4, 8, 128), F32),
                pltpu.VMEM((4, 2, 24, 128), F32),
                pltpu.VMEM((2, 32, 128), F32),
                pltpu.VMEM((24, 128), F32),
                pltpu.VMEM((2, slots, 8, 128), F32),
                dma((3 + n_modes, 2)),
                dma((4, 8)),
                dma((4, 8)),
                dma((2, slots)),
                dma((2, slots)),
            ],
            compiler_params=pltpu.CompilerParams(
                collective_id=0, has_side_effects=True, vmem_limit_bytes=VMEM_LIMIT
            ),
        )(
            *(
                pltpu.with_memory_space_constraint(v, pltpu.HBM)
                for v in (mode_scale, forcing, metric, jacobian)
            )
        )
        return tuple(jnp.swapaxes(o, 1, 2).reshape(forcing.shape) for o in outs)

    return jax.shard_map(
        step,
        mesh=mesh,
        in_specs=(P(None, "curve", "sub"), P("curve", "sub"), P("curve", "sub"), P()),
        out_specs=(P(None, "curve", "sub"), P(None, "curve", "sub")),
        check_vma=False,
    )
```

```python
import functools
import math

import jax
import jax.numpy as jnp
import numpy as np
from jax import lax
from jax.experimental import pallas as pl
from jax.experimental.pallas import tpu as pltpu
from jax.sharding import PartitionSpec as P

MESH = pl.DeviceIdType.MESH
EDGES = ((0, 1), (0, 2), (0, 3), (1, 2), (1, 3), (2, 3))
F32 = jnp.float32
VMEM_LIMIT = 40 * 1024 * 1024


def gll_slopes():
    points = np.array([-1.0, -1.0 / math.sqrt(5.0), 1.0 / math.sqrt(5.0), 1.0])
    factor = np.array(
        [np.prod([points[j] - points[m] for m in range(4) if m != j]) for j in range(4)]
    )
    slopes = np.zeros((4, 4))
    for i in range(4):
        for j in range(4):
            if i != j:
                slopes[i, j] = factor[i] / (factor[j] * (points[i] - points[j]))
        slopes[i, i] = sum((1.0 / (points[i] - points[m]) for m in range(4) if m != i))
    return slopes


def kernel(
    cfg,
    scale_hbm,
    f_hbm,
    met_hbm,
    jac_hbm,
    x_ref,
    r_ref,
    scale_ref,
    fbuf,
    metbuf,
    jacbuf,
    w0,
    w1,
    w2,
    w3,
    y0,
    y1,
    y2,
    minv,
    nat,
    mass,
    cx,
    cy,
    perm,
    edge,
    dots,
    rowbuf,
    cornbuf,
    colbuf,
    rowrecv,
    cornrecv,
    colrecv,
    rowfix,
    colfix,
    red,
    in_sems,
    send_sems,
    recv_sems,
    rs_send,
    rs_recv,
):
    n_modes, n_curve, n_sub, n_zc = cfg
    n_pairs = n_modes // 2
    n_y = n_curve // n_zc
    c = lax.axis_index("curve")
    s = lax.axis_index("sub")
    c_prev, c_next = lax.rem(c + n_curve - 1, n_curve), lax.rem(c + 1, n_curve)
    s_prev, s_next = lax.rem(s + n_sub - 1, n_sub), lax.rem(s + 1, n_sub)
    y_pos, zc_pos = c // n_zc, lax.rem(c, n_zc)
    b_size = n_y * n_sub
    b_pos = y_pos * n_sub + s

    halves = (pl.ds(0, 128), pl.ds(128, 128))
    loads = []
    for h in range(2):
        loads.append(pltpu.make_async_copy(met_hbm.at[:, halves[h]], metbuf.at[h], in_sems.at[0, h]))
        loads.append(pltpu.make_async_copy(jac_hbm.at[:, halves[h]], jacbuf.at[h], in_sems.at[1, h]))
    for m in range(n_modes):
        for h in range(2):
            loads.append(
                pltpu.make_async_copy(f_hbm.at[m, :, halves[h]], fbuf.at[m, h], in_sems.at[2 + m, h])
            )
    loads.append(pltpu.make_async_copy(scale_hbm, scale_ref, in_sems.at[2 + n_modes, 0]))
    for load in loads:
        load.start()

    def a_member(d):
        pos = lax.rem(zc_pos + d, n_zc)
        return (y_pos * n_zc + pos, s)

    def b_member(d):
        pos = lax.rem(b_pos + d, b_size)
        return ((pos // n_sub) * n_zc + zc_pos, lax.rem(pos, n_sub))

    around = [
        (c_prev, s), (c_next, s), (c, s_prev), (c, s_next),
        (c_prev, s_prev), (c_prev, s_next), (c_next, s_prev), (c_next, s_next),
    ]
    partners = around + [a_member(d) for d in range(1, n_zc)] + [b_member(d) for d in range(1, b_size)]
    barrier = pltpu.get_barrier_semaphore()
    for device in partners:
        pl.semaphore_signal(barrier, inc=1, device_id=device, device_id_type=MESH)

    def lanes_of(rows):
        return lax.broadcasted_iota(jnp.int32, (rows, 128), 1)

    def rows_of(rows):
        return lax.broadcasted_iota(jnp.int32, (rows, 128), 0)

    lane, subl = lanes_of(8), rows_of(8)
    at_low, at_high, low_half = (lane & 63) == 0, (lane & 63) == 63, lane < 64
    slopes = gll_slopes()
    weights = (1.0 / 6.0, 5.0 / 6.0, 5.0 / 6.0, 1.0 / 6.0)

    big_r = lax.broadcasted_iota(jnp.int32, (256, 256), 0)
    big_c = lax.broadcasted_iota(jnp.int32, (256, 256), 1)
    for odd in range(2):
        into = ((big_r & 3) ^ odd) * 64 + (big_r >> 2) == big_c
        perm[odd] = jnp.where(into, 1.0, 0.0).astype(jnp.bfloat16)

    def select_exact(x, which):
        high = x.astype(jnp.bfloat16)
        rest = x - high.astype(F32)
        mid = rest.astype(jnp.bfloat16)
        low = (rest - mid.astype(F32)).astype(jnp.bfloat16)
        matrix = perm[which]

        def dot(part):
            return jnp.dot(part, matrix, preferred_element_type=F32)

        return (dot(high) + dot(mid)) + dot(low)

    def natural(buf):
        return jnp.concatenate(
            [
                jnp.concatenate([buf[h, pl.ds(a, 24, stride=4), :] for a in range(4)], axis=0)
                for h in range(2)
            ],
            axis=1,
        )

    def deinterleave(x_even, x_odd):
        lo = lanes_of(x_even.shape[0]) < 64
        even, odd = select_exact(x_even, 0), select_exact(x_odd, 1)
        out = []
        for q in range(2):
            e, o = even[:, 128 * q : 128 * (q + 1)], odd[:, 128 * q : 128 * (q + 1)]
            out.append(jnp.where(lo, e, o))
            out.append(pltpu.roll(jnp.where(lo, o, e), 64, 1))
        return out

    def to_natural(slot, planes, p):
        lo = lanes_of(96) < 64
        full = [jnp.concatenate([planes[p, a, b] for a in range(4)], axis=0) for b in range(4)]
        odd1, odd3 = pltpu.roll(full[1], 64, 1), pltpu.roll(full[3], 64, 1)
        even = jnp.concatenate([jnp.where(lo, full[0], odd1), jnp.where(lo, full[2], odd3)], axis=1)
        odd = jnp.concatenate([jnp.where(lo, odd1, full[0]), jnp.where(lo, odd3, full[2])], axis=1)
        for par, packed in enumerate((even, odd)):
            out = select_exact(packed, 2 + par)
            for h in range(2):
                nat[slot, 2 * p + par, h] = out[:, 128 * h : 128 * (h + 1)]

    for load in loads[:4]:
        load.wait()
    for target, buf in ((mass, jacbuf), (minv, metbuf)):
        x = natural(buf)
        for b, plane in enumerate(deinterleave(x, x)):
            for a in range(4):
                grid_w = F32(weights[a]) * F32(weights[b])
                value = plane[24 * a : 24 * (a + 1)] * grid_w
                if target is mass:
                    mass[a, b] = value
                else:
                    minv[0, a, b] = value

    def setup(t, carry):
        rows = pl.ds(pl.multiple_of(t * 8, 8), 8)
        flux = [[minv[0, a, b, rows, :] for b in range(4)] for a in range(4)]

        def mix(values, table):
            total = values[0] * F32(table[0])
            for q in range(1, 4):
                total = total + values[q] * F32(table[q])
            return total

        for b in range(4):
            column = [flux[q][b] for q in range(4)]
            for e, (i, j) in enumerate(EDGES):
                table = slopes[:, i] * slopes[:, j]
                cx[e, b, rows, :] = mix(column, table)
                cy[e, b, rows, :] = mix(flux[b], table)
            for a in range(4):
                lap = mix(column, slopes[:, a] ** 2) + mix(flux[a], slopes[:, b] ** 2)
                w0[n_pairs, a, b, rows, :] = jnp.where(low_half, mass[a, b, rows, :], lap)
        return carry

    lax.fori_loop(0, 3, setup, 0)
    dots[...] = jnp.zeros_like(dots)
    rowbuf[...] = jnp.zeros_like(rowbuf)
    cornbuf[...] = jnp.zeros_like(cornbuf)

    lane24, row24 = lanes_of(24), rows_of(24)
    low_end = (lane24 & 63) == 0
    pack_key = ((lane24 + 1) & 63) >> 1
    pack_key2 = ((lane24 + 1) & 127) >> 1

    def row_join(w, p):
        for b in range(4):
            top, bottom = w[p, 0, b], w[p, 3, b]
            w[p, 3, b] = bottom + jnp.where(row24 < 23, pltpu.roll(top, 23, 0), 0.0)
            w[p, 0, b] = top + jnp.where(row24 > 0, pltpu.roll(bottom, 1, 0), 0.0)

    def col_join(w, p):
        inner_high, inner_low = lane24 & 63 != 63, lane24 & 63 != 0
        for a in range(4):
            first, last = w[p, a, 0], w[p, a, 3]
            w[p, a, 3] = last + jnp.where(inner_high, pltpu.roll(first, 127, 1), 0.0)
            w[p, a, 0] = first + jnp.where(inner_low, pltpu.roll(last, 1, 1), 0.0)

    def pack_cols(w, p, packed):
        for a in range(4):
            k = 4 * p + a
            ends = jnp.where(low_end, w[p, a, 0], w[p, a, 3])
            ends = pltpu.roll(ends, 2 * k, 1) if k else ends
            packed = jnp.where(pack_key == k, ends, packed)
        return packed

    def put_row(e, side, p, lines):
        for b in range(4):
            rowbuf[e, side, 8 * b + p : 8 * b + p + 1, :] = lines[b]

    def put_corners(e, side):
        cornbuf[e, side] = jnp.where(at_low, rowbuf[e, side, 0:8, :], rowbuf[e, side, 24:32, :])

    def copies(e):
        plan = [
            (rowbuf.at[e, 1], rowrecv.at[e, 0], (c_next, s)),
            (rowbuf.at[e, 0], rowrecv.at[e, 1], (c_prev, s)),
            (colbuf.at[e], colrecv.at[e, 0], (c, s_next)),
            (colbuf.at[e], colrecv.at[e, 1], (c, s_prev)),
            (cornbuf.at[e, 1], cornrecv.at[e, 0], (c_next, s_next)),
            (cornbuf.at[e, 1], cornrecv.at[e, 1], (c_next, s_prev)),
            (cornbuf.at[e, 0], cornrecv.at[e, 2], (c_prev, s_next)),
            (cornbuf.at[e, 0], cornrecv.at[e, 3], (c_prev, s_prev)),
        ]
        return [
            pltpu.make_async_remote_copy(
                src_ref=src,
                dst_ref=dst,
                send_sem=send_sems.at[e, i],
                recv_sem=recv_sems.at[e, i],
                device_id=device,
                device_id_type=MESH,
            )
            for i, (src, dst, device) in enumerate(plan)
        ]

    def send_rows(sent, e, side):
        put_corners(e, side)
        for i in (6, 7, 1) if side == 0 else (4, 5, 0):
            sent[i].start()

    def send_cols(sent, e, w):
        packed = jnp.zeros((24, 128), F32)
        for p in range(n_pairs):
            row_join(w, p)
            packed = pack_cols(w, p, packed)
        colbuf[e] = packed
        for copy in sent[2:4]:
            copy.start()
        for p in range(n_pairs):
            col_join(w, p)

    def first_exchange():
        sent = copies(0)
        edge[...] = jnp.zeros_like(edge)
        for load in loads[4:-1]:
            load.wait()
        for m in range(n_modes):
            for h in range(2):
                for side in range(2):
                    r, i = 8 * side + m // 2, 95 * side
                    edge[m % 2, h, r : r + 1, :] = fbuf[m, h, i : i + 1, :]
        planes = deinterleave(
            *(jnp.concatenate([edge[par, 0], edge[par, 1]], axis=1) for par in range(2))
        )
        for side in range(2):
            for b in range(4):
                line = mass[0, b, 0:1, :] if side == 0 else mass[3, b, 23:24, :]
                rowbuf[0, side, 8 * b : 8 * b + 8, :] = planes[b][8 * side : 8 * side + 8] * line
        put_row(0, 0, n_pairs, [w0[n_pairs, 0, b, 0:1, :] for b in range(4)])
        put_row(0, 1, n_pairs, [w0[n_pairs, 3, b, 23:24, :] for b in range(4)])
        pl.semaphore_wait(barrier, len(partners))
        send_rows(sent, 0, 0)
        send_rows(sent, 0, 1)
        packed = jnp.zeros((24, 128), F32)
        for a in range(4):
            every = pl.ds(a, 24, stride=4)
            grid_w = F32(weights[a]) * F32(weights[0])
            ends_mass = jnp.where(lane24 == 127, jacbuf[1, every, :], jacbuf[0, every, :]) * grid_w
            for p in range(n_pairs):
                for par in range(2):
                    k = 4 * p + a + 32 * par
                    ends = jnp.where(
                        lane24 == 127, fbuf[2 * p + 1 - par, 1, every, :], fbuf[2 * p + par, 0, every, :]
                    )
                    ends = ends * ends_mass
                    ends = pltpu.roll(ends, 2 * k, 1) if k else ends
                    packed = jnp.where(pack_key2 == k, ends, packed)
        below = pltpu.roll(pltpu.roll(packed, 6, 1), 23, 0)
        above = pltpu.roll(pltpu.roll(packed, 122, 1), 1, 0)
        packed = (
            packed
            + jnp.where(((pack_key & 3) == 3) & (row24 < 23), below, 0.0)
            + jnp.where(((pack_key & 3) == 0) & (row24 > 0), above, 0.0)
        )
        row_join(w0, n_pairs)
        colbuf[0] = pack_cols(w0, n_pairs, packed)
        for copy in sent[2:4]:
            copy.start()
        for p in range(n_pairs):
            planes = deinterleave(natural(fbuf.at[2 * p]), natural(fbuf.at[2 * p + 1]))
            for b in range(4):
                for a in range(4):
                    w0[p, a, b] = planes[b][24 * a : 24 * (a + 1)] * mass[a, b]
            row_join(w0, p)
            col_join(w0, p)
        col_join(w0, n_pairs)
        for odd in range(2):
            back = ((big_c & 3) ^ odd) * 64 + (big_c >> 2) == big_r
            perm[2 + odd] = jnp.where(back, 1.0, 0.0).astype(jnp.bfloat16)
        loads[-1].wait()
        return sent

    def arrive_cols(e, sent):
        for copy in sent[2:4]:
            copy.wait_recv()
        colfix[...] = jnp.where(
            (lane24 & 1) == 0, pltpu.roll(colrecv[e, 0], 65, 1), pltpu.roll(colrecv[e, 1], 63, 1)
        )

    def arrive_rows(e, sent):
        for copy in sent[:2] + sent[4:]:
            copy.wait_recv()
        for side in range(2):
            r = [rowrecv[e, side, 8 * b : 8 * b + 8, :] for b in range(4)]
            left = pltpu.roll(cornrecv[e, 2 * side], 65, 1)
            right = pltpu.roll(cornrecv[e, 2 * side + 1], 63, 1)
            rowfix[side, 0:8, :] = r[0] + jnp.where(at_low, left, pltpu.roll(r[3], 1, 1))
            rowfix[side, 8:16, :] = r[1]
            rowfix[side, 16:24, :] = r[2]
            rowfix[side, 24:32, :] = r[3] + jnp.where(at_high, right, pltpu.roll(r[0], 127, 1))

    def fixed(w, p, r0, outer):
        rows = pl.ds(r0, 8)
        out = []
        for a in range(4):
            k = 4 * p + a
            ends = colfix[rows, :]
            ends = pltpu.roll(ends, (-2 * k) % 128, 1) if k else ends
            line = []
            for b in range(4):
                value = w[p, a, b, rows, :]
                if b == 0:
                    value = value + jnp.where(at_low, ends, 0.0)
                if b == 3:
                    value = value + jnp.where(at_high, ends, 0.0)
                r = 8 * b + p
                if outer and a == 0:
                    value = value + jnp.where(subl + r0 == 0, rowfix[0, r : r + 1, :], 0.0)
                if outer and a == 3:
                    value = value + jnp.where(subl + r0 == 23, rowfix[1, r : r + 1, :], 0.0)
                line.append(value)
            out.append(line)
        return out

    def total(values):
        values = list(values)
        while len(values) > 1:
            values = [
                values[i] + values[i + 1] if i + 1 < len(values) else values[i]
                for i in range(0, len(values), 2)
            ]
        return values[0]

    quad = [(a, b) for a in range(4) for b in range(4)]

    def step(k, w_in, w_out, y_old, y_new, t, outer):
        r0 = 8 * t
        rows = pl.ds(r0, 8)
        if k == 0:
            both = fixed(w_in, n_pairs, r0, outer)
            for a, b in quad:
                swapped = pltpu.roll(both[a][b], 64, 1)
                w_in[n_pairs, a, b, rows, :] = jnp.where(low_half, both[a][b], swapped)
                y2[0, a, b, rows, :] = jnp.where(low_half, swapped, both[a][b])
        for p in range(n_pairs):
            scale = jnp.where(low_half, scale_ref[2 * p], scale_ref[2 * p + 1])
            value = fixed(w_in, p, r0, outer)
            vec = [[None] * 4 for _ in range(4)]
            for a, b in quad:
                w_in[p, a, b, rows, :] = value[a][b]
                if k == 0:
                    diag = w_in[n_pairs, a, b, rows, :] + scale * y2[0, a, b, rows, :]
                    inv = 1.0 / diag
                    minv[p, a, b, rows, :] = inv
                    vec[a][b] = value[a][b] * inv
                else:
                    vec[a][b] = value[a][b] * minv[p, a, b, rows, :] - y_old[p, a, b, rows, :]
                y_new[p, a, b, rows, :] = vec[a][b]
            lap = [[None] * 4 for _ in range(4)]

            def flow(table, e, line, i, j):
                (ai, bi), (aj, bj) = i, j
                f = table[e, line, rows, :] * (vec[aj][bj] - vec[ai][bi])
                lap[ai][bi] = f if lap[ai][bi] is None else lap[ai][bi] + f
                lap[aj][bj] = -f if lap[aj][bj] is None else lap[aj][bj] - f

            for line in range(4):
                for e, (i, j) in enumerate(EDGES):
                    flow(cx, e, line, (i, line), (j, line))
            image = [[None] * 4 for _ in range(4)]
            for a in range(4):
                for e, (i, j) in enumerate(EDGES):
                    flow(cy, e, a, (a, i), (a, j))
                for b in range(4):
                    image[a][b] = mass[a, b, rows, :] * vec[a][b] + scale * lap[a][b]
                    w_out[p, a, b, rows, :] = image[a][b]
            if outer:
                side = t // 2
                put_row(k + 1, side, p, [image[3 * side][b][7 * side : 7 * side + 1] for b in range(4)])
            if k == 0:
                count = (0.5, 1.0, 1.0, 0.5)
                terms = []
                for a, b in quad:
                    term = vec[a][b] * value[a][b]
                    weight = count[a] * count[b]
                    terms.append(term if weight == 1.0 else term * F32(weight))
                dots[0, p] += total(terms)
                dots[1, p] += total(vec[a][b] * image[a][b] for a, b in quad)
            else:
                dots[2 * k, p] += total(y_old[p, a, b, rows, :] * image[a][b] for a, b in quad)
                dots[2 * k + 1, p] += total(vec[a][b] * image[a][b] for a, b in quad)

    def run_step(k, sent, w_in, w_out, y_old, y_new):
        arrive_cols(k, sent)
        step(k, w_in, w_out, y_old, y_new, 1, False)
        arrive_rows(k, sent)
        following = copies(k + 1)
        for side in range(2):
            step(k, w_in, w_out, y_old, y_new, 2 * side, True)
            send_rows(following, k + 1, side)
        return following

    sent0 = first_exchange()
    sent1 = run_step(0, sent0, w0, w1, None, y0)
    send_cols(sent1, 1, w1)
    sent2 = run_step(1, sent1, w1, w2, y0, y1)
    send_cols(sent2, 2, w2)
    sent3 = run_step(2, sent2, w2, w3, y1, y2)

    local = jnp.zeros((8, 128), F32)
    for p in range(n_pairs):
        stacked = jnp.zeros((8, 128), F32)
        for q in range(6):
            stacked = jnp.where(subl == q, jnp.sum(dots[q, p], axis=0, keepdims=True), stacked)
        for par in range(2):
            half = jnp.where(low_half, stacked, 0.0) if par == 0 else jnp.where(low_half, 0.0, stacked)
            local = jnp.where(lane == 2 * p + par, jnp.sum(half, axis=1, keepdims=True), local)

    def phase_start(i, value, size, pos, member):
        red[i, pos] = value
        moves = [
            pltpu.make_async_remote_copy(
                src_ref=red.at[i, pos],
                dst_ref=red.at[i, pos],
                send_sem=rs_send.at[i, d - 1],
                recv_sem=rs_recv.at[i, d - 1],
                device_id=member(d),
                device_id_type=MESH,
            )
            for d in range(1, size)
        ]
        for move in moves:
            move.start()
        return moves

    def phase_end(i, size, moves):
        for move in moves:
            move.wait_recv()
        return total(red[i, j] for j in range(size))

    def run_natural(slot, planes):
        for p in range(n_pairs):
            to_natural(slot, planes, p)

    moves_a = phase_start(0, local, n_zc, zc_pos, a_member)
    send_cols(sent3, 3, w3)
    for slot, planes in enumerate((y0, y1, y2)):
        run_natural(slot, planes)
    moves_b = phase_start(1, phase_end(0, n_zc, moves_a), b_size, b_pos, b_member)
    for slot, planes in enumerate((w0, w1, w2)):
        run_natural(3 + slot, planes)
    arrive_cols(3, sent3)
    arrive_rows(3, sent3)

    def last_fix(t, carry):
        r0 = pl.multiple_of(t * 8, 8)
        for p in range(n_pairs):
            value = fixed(w3, p, r0, True)
            for a, b in quad:
                w3[p, a, b, pl.ds(r0, 8), :] = value[a][b]
        return carry

    lax.fori_loop(0, 3, last_fix, 0)
    run_natural(6, w3)
    g = phase_end(1, b_size, moves_b)

    b0, k00, k01, k11, k12, k22 = (g[q : q + 1, :] for q in range(6))
    k02 = k11
    b1 = k00 - b0
    b2 = k01 - b1
    l10 = k01 / k00
    l20 = k02 / k00
    d1 = k11 - l10 * k01
    e12 = k12 - l10 * k02
    l21 = e12 / d1
    d2 = k22 - l20 * k02 - l21 * e12
    c1 = b1 - l10 * b0
    c2 = b2 - l20 * b0 - l21 * c1
    a2 = c2 / d2
    a1 = c1 / d1 - l21 * a2
    a0 = b0 / k00 - l10 * a1 - l20 * a2

    for m in range(n_modes):
        u0, u1, u2 = (jnp.broadcast_to(v[:, m : m + 1], (8, 128)) for v in (a0, a1, a2))
        for h in range(2):
            for a in range(4):
                for t in range(3):
                    src = pl.ds(24 * a + 8 * t, 8)
                    dst = pl.ds(a + 32 * t, 8, stride=4)
                    n = [nat[i, m, h, src, :] for i in range(7)]
                    x_ref[m, h, dst, :] = u0 * n[0] + u1 * n[1] + u2 * n[2]
                    r_ref[m, h, dst, :] = n[3] - u0 * n[4] - u1 * n[5] - u2 * n[6]
    for group in (sent0, sent1, sent2, sent3, moves_a, moves_b):
        for copy in group:
            copy.wait_send()


def solution(mesh, n_zc=None):
    n_curve, n_sub = mesh.shape["curve"], mesh.shape["sub"]
    n_zc = n_zc or 16
    n_y = n_curve // n_zc

    def step(forcing, metric, jacobian, mode_scale):
        n_modes, n_rows, n_cols = forcing.shape
        n_pairs = n_modes // 2
        vec = pltpu.VMEM((n_pairs, 4, 4, 24, 128), F32)
        dma = pltpu.SemaphoreType.DMA
        cfg = (n_modes, n_curve, n_sub, n_zc)
        out = jax.ShapeDtypeStruct((n_modes, 2, n_rows, 128), F32)
        slots = max(n_zc, n_y * n_sub)
        outs = pl.pallas_call(
            functools.partial(kernel, cfg),
            out_shape=(out, out),
            in_specs=[pl.BlockSpec(memory_space=pltpu.HBM)] * 4,
            out_specs=(pl.BlockSpec(memory_space=pltpu.VMEM),) * 2,
            scratch_shapes=[
                pltpu.SMEM((n_modes,), F32),
                pltpu.VMEM((n_modes, 2, n_rows, 128), F32),
                pltpu.VMEM((2, n_rows, 128), F32),
                pltpu.VMEM((2, n_rows, 128), F32),
                pltpu.VMEM((n_pairs + 1, 4, 4, 24, 128), F32),
                vec, vec, vec, vec, vec, vec, vec,
                pltpu.VMEM((7, n_modes, 2, n_rows, 128), F32),
                pltpu.VMEM((4, 4, 24, 128), F32),
                pltpu.VMEM((6, 4, 24, 128), F32),
                pltpu.VMEM((6, 4, 24, 128), F32),
                pltpu.VMEM((4, 256, 256), jnp.bfloat16),
                pltpu.VMEM((2, 2, 16, 128), F32),
                pltpu.VMEM((6, n_pairs, 8, 128), F32),
                pltpu.VMEM((4, 2, 32, 128), F32),
                pltpu.VMEM((4, 2, 8, 128), F32),
                pltpu.VMEM((4, 24, 128), F32),
                pltpu.VMEM((4, 2, 32, 128), F32),
                pltpu.VMEM((4, 4, 8, 128), F32),
                pltpu.VMEM((4, 2, 24, 128), F32),
                pltpu.VMEM((2, 32, 128), F32),
                pltpu.VMEM((24, 128), F32),
                pltpu.VMEM((2, slots, 8, 128), F32),
                dma((3 + n_modes, 2)),
                dma((4, 8)),
                dma((4, 8)),
                dma((2, slots)),
                dma((2, slots)),
            ],
            compiler_params=pltpu.CompilerParams(
                collective_id=0, has_side_effects=True, vmem_limit_bytes=VMEM_LIMIT
            ),
        )(
            *(
                pltpu.with_memory_space_constraint(v, pltpu.HBM)
                for v in (mode_scale, forcing, metric, jacobian)
            )
        )
        return tuple(jnp.swapaxes(o, 1, 2).reshape(forcing.shape) for o in outs)

    return jax.shard_map(
        step,
        mesh=mesh,
        in_specs=(P(None, "curve", "sub"), P("curve", "sub"), P("curve", "sub"), P()),
        out_specs=(P(None, "curve", "sub"), P(None, "curve", "sub")),
        check_vma=False,
    )
```

```python
import functools
import math

import jax
import jax.numpy as jnp
import numpy as np
from jax import lax
from jax.experimental import pallas as pl
from jax.experimental.pallas import tpu as pltpu
from jax.sharding import PartitionSpec as P

MESH = pl.DeviceIdType.MESH
EDGES = ((0, 1), (0, 2), (0, 3), (1, 2), (1, 3), (2, 3))
F32 = jnp.float32
VMEM_LIMIT = 40 * 1024 * 1024


def gll_slopes():
    points = np.array([-1.0, -1.0 / math.sqrt(5.0), 1.0 / math.sqrt(5.0), 1.0])
    factor = np.array(
        [np.prod([points[j] - points[m] for m in range(4) if m != j]) for j in range(4)]
    )
    slopes = np.zeros((4, 4))
    for i in range(4):
        for j in range(4):
            if i != j:
                slopes[i, j] = factor[i] / (factor[j] * (points[i] - points[j]))
        slopes[i, i] = sum((1.0 / (points[i] - points[m]) for m in range(4) if m != i))
    return slopes


def kernel(
    cfg,
    scale_hbm,
    f_hbm,
    met_hbm,
    jac_hbm,
    x_ref,
    r_ref,
    scale_ref,
    fbuf,
    metbuf,
    jacbuf,
    w0,
    w1,
    w2,
    w3,
    y0,
    y1,
    y2,
    minv,
    nat,
    mass,
    cx,
    cy,
    perm,
    edge,
    dots,
    rowbuf,
    cornbuf,
    colbuf,
    rowrecv,
    cornrecv,
    colrecv,
    rowfix,
    colfix,
    red,
    in_sems,
    send_sems,
    recv_sems,
    rs_send,
    rs_recv,
):
    n_modes, n_curve, n_sub, n_zc = cfg
    n_pairs = n_modes // 2
    n_y = n_curve // n_zc
    c = lax.axis_index("curve")
    s = lax.axis_index("sub")
    c_prev, c_next = lax.rem(c + n_curve - 1, n_curve), lax.rem(c + 1, n_curve)
    s_prev, s_next = lax.rem(s + n_sub - 1, n_sub), lax.rem(s + 1, n_sub)
    y_pos, zc_pos = c // n_zc, lax.rem(c, n_zc)
    b_size = n_y * n_sub
    b_pos = y_pos * n_sub + s

    halves = (pl.ds(0, 128), pl.ds(128, 128))
    loads = []
    for h in range(2):
        loads.append(pltpu.make_async_copy(met_hbm.at[:, halves[h]], metbuf.at[h], in_sems.at[0, h]))
        loads.append(pltpu.make_async_copy(jac_hbm.at[:, halves[h]], jacbuf.at[h], in_sems.at[1, h]))
    for m in range(n_modes):
        for h in range(2):
            loads.append(
                pltpu.make_async_copy(f_hbm.at[m, :, halves[h]], fbuf.at[m, h], in_sems.at[2 + m, h])
            )
    loads.append(pltpu.make_async_copy(scale_hbm, scale_ref, in_sems.at[2 + n_modes, 0]))
    for load in loads:
        load.start()

    def a_member(d):
        pos = lax.rem(zc_pos + d, n_zc)
        return (y_pos * n_zc + pos, s)

    def b_member(d):
        pos = lax.rem(b_pos + d, b_size)
        return ((pos // n_sub) * n_zc + zc_pos, lax.rem(pos, n_sub))

    around = [
        (c_prev, s), (c_next, s), (c, s_prev), (c, s_next),
        (c_prev, s_prev), (c_prev, s_next), (c_next, s_prev), (c_next, s_next),
    ]
    partners = around + [a_member(d) for d in range(1, n_zc)] + [b_member(d) for d in range(1, b_size)]
    barrier = pltpu.get_barrier_semaphore()
    for device in partners:
        pl.semaphore_signal(barrier, inc=1, device_id=device, device_id_type=MESH)

    def lanes_of(rows):
        return lax.broadcasted_iota(jnp.int32, (rows, 128), 1)

    def rows_of(rows):
        return lax.broadcasted_iota(jnp.int32, (rows, 128), 0)

    lane, subl = lanes_of(8), rows_of(8)
    at_low, at_high, low_half = (lane & 63) == 0, (lane & 63) == 63, lane < 64
    slopes = gll_slopes()
    weights = (1.0 / 6.0, 5.0 / 6.0, 5.0 / 6.0, 1.0 / 6.0)

    big_r = lax.broadcasted_iota(jnp.int32, (256, 256), 0)
    big_c = lax.broadcasted_iota(jnp.int32, (256, 256), 1)
    for odd in range(2):
        into = ((big_r & 3) ^ odd) * 64 + (big_r >> 2) == big_c
        perm[odd] = jnp.where(into, 1.0, 0.0).astype(jnp.bfloat16)

    def select_exact(x, which):
        high = x.astype(jnp.bfloat16)
        rest = x - high.astype(F32)
        mid = rest.astype(jnp.bfloat16)
        low = (rest - mid.astype(F32)).astype(jnp.bfloat16)
        matrix = perm[which]

        def dot(part):
            return jnp.dot(part, matrix, preferred_element_type=F32)

        return (dot(high) + dot(mid)) + dot(low)

    def natural(buf):
        return jnp.concatenate(
            [
                jnp.concatenate([buf[h, pl.ds(a, 24, stride=4), :] for a in range(4)], axis=0)
                for h in range(2)
            ],
            axis=1,
        )

    def deinterleave(x_even, x_odd):
        lo = lanes_of(x_even.shape[0]) < 64
        even, odd = select_exact(x_even, 0), select_exact(x_odd, 1)
        out = []
        for q in range(2):
            e, o = even[:, 128 * q : 128 * (q + 1)], odd[:, 128 * q : 128 * (q + 1)]
            out.append(jnp.where(lo, e, o))
            out.append(pltpu.roll(jnp.where(lo, o, e), 64, 1))
        return out

    def to_natural(slot, planes, p):
        lo = lanes_of(96) < 64
        full = [jnp.concatenate([planes[p, a, b] for a in range(4)], axis=0) for b in range(4)]
        odd1, odd3 = pltpu.roll(full[1], 64, 1), pltpu.roll(full[3], 64, 1)
        even = jnp.concatenate([jnp.where(lo, full[0], odd1), jnp.where(lo, full[2], odd3)], axis=1)
        odd = jnp.concatenate([jnp.where(lo, odd1, full[0]), jnp.where(lo, odd3, full[2])], axis=1)
        for par, packed in enumerate((even, odd)):
            out = select_exact(packed, 2 + par)
            for h in range(2):
                nat[slot, 2 * p + par, h] = out[:, 128 * h : 128 * (h + 1)]

    for load in loads[:4]:
        load.wait()
    for target, buf in ((mass, jacbuf), (minv, metbuf)):
        x = natural(buf)
        for b, plane in enumerate(deinterleave(x, x)):
            for a in range(4):
                grid_w = F32(weights[a]) * F32(weights[b])
                value = plane[24 * a : 24 * (a + 1)] * grid_w
                if target is mass:
                    mass[a, b] = value
                else:
                    minv[0, a, b] = value

    def setup(t, carry):
        rows = pl.ds(pl.multiple_of(t * 8, 8), 8)
        flux = [[minv[0, a, b, rows, :] for b in range(4)] for a in range(4)]

        def mix(values, table):
            total = values[0] * F32(table[0])
            for q in range(1, 4):
                total = total + values[q] * F32(table[q])
            return total

        for b in range(4):
            column = [flux[q][b] for q in range(4)]
            for e, (i, j) in enumerate(EDGES):
                table = slopes[:, i] * slopes[:, j]
                cx[e, b, rows, :] = mix(column, table)
                cy[e, b, rows, :] = mix(flux[b], table)
            for a in range(4):
                lap = mix(column, slopes[:, a] ** 2) + mix(flux[a], slopes[:, b] ** 2)
                w0[n_pairs, a, b, rows, :] = jnp.where(low_half, mass[a, b, rows, :], lap)
        return carry

    lax.fori_loop(0, 3, setup, 0)
    dots[...] = jnp.zeros_like(dots)
    rowbuf[...] = jnp.zeros_like(rowbuf)
    cornbuf[...] = jnp.zeros_like(cornbuf)

    lane24, row24 = lanes_of(24), rows_of(24)
    low_end = (lane24 & 63) == 0
    pack_key = ((lane24 + 1) & 63) >> 1
    pack_key2 = ((lane24 + 1) & 127) >> 1

    def row_join(w, p):
        for b in range(4):
            top, bottom = w[p, 0, b], w[p, 3, b]
            w[p, 3, b] = bottom + jnp.where(row24 < 23, pltpu.roll(top, 23, 0), 0.0)
            w[p, 0, b] = top + jnp.where(row24 > 0, pltpu.roll(bottom, 1, 0), 0.0)

    def col_join(w, p):
        inner_high, inner_low = lane24 & 63 != 63, lane24 & 63 != 0
        for a in range(4):
            first, last = w[p, a, 0], w[p, a, 3]
            w[p, a, 3] = last + jnp.where(inner_high, pltpu.roll(first, 127, 1), 0.0)
            w[p, a, 0] = first + jnp.where(inner_low, pltpu.roll(last, 1, 1), 0.0)

    def pack_cols(w, p, packed):
        for a in range(4):
            k = 4 * p + a
            ends = jnp.where(low_end, w[p, a, 0], w[p, a, 3])
            ends = pltpu.roll(ends, 2 * k, 1) if k else ends
            packed = jnp.where(pack_key == k, ends, packed)
        return packed

    def put_row(e, side, p, lines):
        for b in range(4):
            rowbuf[e, side, 8 * b + p : 8 * b + p + 1, :] = lines[b]

    def put_corners(e, side):
        cornbuf[e, side] = jnp.where(at_low, rowbuf[e, side, 0:8, :], rowbuf[e, side, 24:32, :])

    def copies(e):
        plan = [
            (rowbuf.at[e, 1], rowrecv.at[e, 0], (c_next, s)),
            (rowbuf.at[e, 0], rowrecv.at[e, 1], (c_prev, s)),
            (colbuf.at[e], colrecv.at[e, 0], (c, s_next)),
            (colbuf.at[e], colrecv.at[e, 1], (c, s_prev)),
            (cornbuf.at[e, 1], cornrecv.at[e, 0], (c_next, s_next)),
            (cornbuf.at[e, 1], cornrecv.at[e, 1], (c_next, s_prev)),
            (cornbuf.at[e, 0], cornrecv.at[e, 2], (c_prev, s_next)),
            (cornbuf.at[e, 0], cornrecv.at[e, 3], (c_prev, s_prev)),
        ]
        return [
            pltpu.make_async_remote_copy(
                src_ref=src,
                dst_ref=dst,
                send_sem=send_sems.at[e, i],
                recv_sem=recv_sems.at[e, i],
                device_id=device,
                device_id_type=MESH,
            )
            for i, (src, dst, device) in enumerate(plan)
        ]

    def send_rows(sent, e, side):
        put_corners(e, side)
        for i in (6, 7, 1) if side == 0 else (4, 5, 0):
            sent[i].start()

    def send_cols(sent, e, w):
        packed = jnp.zeros((24, 128), F32)
        for p in range(n_pairs):
            row_join(w, p)
            packed = pack_cols(w, p, packed)
        colbuf[e] = packed
        for copy in sent[2:4]:
            copy.start()
        for p in range(n_pairs):
            col_join(w, p)

    def first_exchange():
        sent = copies(0)
        edge[...] = jnp.zeros_like(edge)
        for load in loads[4:-1]:
            load.wait()
        for m in range(n_modes):
            for h in range(2):
                for side in range(2):
                    r, i = 8 * side + m // 2, 95 * side
                    edge[m % 2, h, r : r + 1, :] = fbuf[m, h, i : i + 1, :]
        planes = deinterleave(
            *(jnp.concatenate([edge[par, 0], edge[par, 1]], axis=1) for par in range(2))
        )
        for side in range(2):
            for b in range(4):
                line = mass[0, b, 0:1, :] if side == 0 else mass[3, b, 23:24, :]
                rowbuf[0, side, 8 * b : 8 * b + 8, :] = planes[b][8 * side : 8 * side + 8] * line
        put_row(0, 0, n_pairs, [w0[n_pairs, 0, b, 0:1, :] for b in range(4)])
        put_row(0, 1, n_pairs, [w0[n_pairs, 3, b, 23:24, :] for b in range(4)])
        pl.semaphore_wait(barrier, len(partners))
        send_rows(sent, 0, 0)
        send_rows(sent, 0, 1)
        packed = jnp.zeros((24, 128), F32)
        for a in range(4):
            every = pl.ds(a, 24, stride=4)
            grid_w = F32(weights[a]) * F32(weights[0])
            ends_mass = jnp.where(lane24 == 127, jacbuf[1, every, :], jacbuf[0, every, :]) * grid_w
            for p in range(n_pairs):
                for par in range(2):
                    k = 4 * p + a + 32 * par
                    ends = jnp.where(
                        lane24 == 127, fbuf[2 * p + 1 - par, 1, every, :], fbuf[2 * p + par, 0, every, :]
                    )
                    ends = ends * ends_mass
                    ends = pltpu.roll(ends, 2 * k, 1) if k else ends
                    packed = jnp.where(pack_key2 == k, ends, packed)
        below = pltpu.roll(pltpu.roll(packed, 6, 1), 23, 0)
        above = pltpu.roll(pltpu.roll(packed, 122, 1), 1, 0)
        packed = (
            packed
            + jnp.where(((pack_key & 3) == 3) & (row24 < 23), below, 0.0)
            + jnp.where(((pack_key & 3) == 0) & (row24 > 0), above, 0.0)
        )
        row_join(w0, n_pairs)
        colbuf[0] = pack_cols(w0, n_pairs, packed)
        for copy in sent[2:4]:
            copy.start()
        for p in range(n_pairs):
            planes = deinterleave(natural(fbuf.at[2 * p]), natural(fbuf.at[2 * p + 1]))
            for b in range(4):
                for a in range(4):
                    w0[p, a, b] = planes[b][24 * a : 24 * (a + 1)] * mass[a, b]
            row_join(w0, p)
            col_join(w0, p)
        col_join(w0, n_pairs)
        for odd in range(2):
            back = ((big_c & 3) ^ odd) * 64 + (big_c >> 2) == big_r
            perm[2 + odd] = jnp.where(back, 1.0, 0.0).astype(jnp.bfloat16)
        loads[-1].wait()
        return sent

    def arrive_cols(e, sent):
        for copy in sent[2:4]:
            copy.wait_recv()
        colfix[...] = jnp.where(
            (lane24 & 1) == 0, pltpu.roll(colrecv[e, 0], 65, 1), pltpu.roll(colrecv[e, 1], 63, 1)
        )

    def arrive_rows(e, sent):
        for copy in sent[:2] + sent[4:]:
            copy.wait_recv()
        for side in range(2):
            r = [rowrecv[e, side, 8 * b : 8 * b + 8, :] for b in range(4)]
            left = pltpu.roll(cornrecv[e, 2 * side], 65, 1)
            right = pltpu.roll(cornrecv[e, 2 * side + 1], 63, 1)
            rowfix[side, 0:8, :] = r[0] + jnp.where(at_low, left, pltpu.roll(r[3], 1, 1))
            rowfix[side, 8:16, :] = r[1]
            rowfix[side, 16:24, :] = r[2]
            rowfix[side, 24:32, :] = r[3] + jnp.where(at_high, right, pltpu.roll(r[0], 127, 1))

    def fixed(w, p, r0, outer):
        rows = pl.ds(r0, 8)
        out = []
        for a in range(4):
            k = 4 * p + a
            ends = colfix[rows, :]
            ends = pltpu.roll(ends, (-2 * k) % 128, 1) if k else ends
            line = []
            for b in range(4):
                value = w[p, a, b, rows, :]
                if b == 0:
                    value = value + jnp.where(at_low, ends, 0.0)
                if b == 3:
                    value = value + jnp.where(at_high, ends, 0.0)
                r = 8 * b + p
                if outer and a == 0:
                    value = value + jnp.where(subl + r0 == 0, rowfix[0, r : r + 1, :], 0.0)
                if outer and a == 3:
                    value = value + jnp.where(subl + r0 == 23, rowfix[1, r : r + 1, :], 0.0)
                line.append(value)
            out.append(line)
        return out

    def total(values):
        values = list(values)
        while len(values) > 1:
            values = [
                values[i] + values[i + 1] if i + 1 < len(values) else values[i]
                for i in range(0, len(values), 2)
            ]
        return values[0]

    quad = [(a, b) for a in range(4) for b in range(4)]

    def step(k, w_in, w_out, y_old, y_new, t, outer):
        r0 = 8 * t
        rows = pl.ds(r0, 8)
        if k == 0:
            both = fixed(w_in, n_pairs, r0, outer)
            for a, b in quad:
                swapped = pltpu.roll(both[a][b], 64, 1)
                w_in[n_pairs, a, b, rows, :] = jnp.where(low_half, both[a][b], swapped)
                y2[0, a, b, rows, :] = jnp.where(low_half, swapped, both[a][b])
        for p in range(n_pairs):
            scale = jnp.where(low_half, scale_ref[2 * p], scale_ref[2 * p + 1])
            value = fixed(w_in, p, r0, outer)
            vec = [[None] * 4 for _ in range(4)]
            for a, b in quad:
                w_in[p, a, b, rows, :] = value[a][b]
                if k == 0:
                    diag = w_in[n_pairs, a, b, rows, :] + scale * y2[0, a, b, rows, :]
                    inv = 1.0 / diag
                    minv[p, a, b, rows, :] = inv
                    vec[a][b] = value[a][b] * inv
                else:
                    vec[a][b] = value[a][b] * minv[p, a, b, rows, :] - y_old[p, a, b, rows, :]
                y_new[p, a, b, rows, :] = vec[a][b]
            lap = [[None] * 4 for _ in range(4)]

            def flow(table, e, line, i, j):
                (ai, bi), (aj, bj) = i, j
                f = table[e, line, rows, :] * (vec[aj][bj] - vec[ai][bi])
                lap[ai][bi] = f if lap[ai][bi] is None else lap[ai][bi] + f
                lap[aj][bj] = -f if lap[aj][bj] is None else lap[aj][bj] - f

            for line in range(4):
                for e, (i, j) in enumerate(EDGES):
                    flow(cx, e, line, (i, line), (j, line))
            image = [[None] * 4 for _ in range(4)]
            for a in range(4):
                for e, (i, j) in enumerate(EDGES):
                    flow(cy, e, a, (a, i), (a, j))
                for b in range(4):
                    image[a][b] = mass[a, b, rows, :] * vec[a][b] + scale * lap[a][b]
                    w_out[p, a, b, rows, :] = image[a][b]
            if outer:
                side = t // 2
                put_row(k + 1, side, p, [image[3 * side][b][7 * side : 7 * side + 1] for b in range(4)])
            if k == 0:
                count = (0.5, 1.0, 1.0, 0.5)
                terms = []
                for a, b in quad:
                    term = vec[a][b] * value[a][b]
                    weight = count[a] * count[b]
                    terms.append(term if weight == 1.0 else term * F32(weight))
                dots[0, p] += total(terms)
                dots[1, p] += total(vec[a][b] * image[a][b] for a, b in quad)
            else:
                dots[2 * k, p] += total(y_old[p, a, b, rows, :] * image[a][b] for a, b in quad)
                dots[2 * k + 1, p] += total(vec[a][b] * image[a][b] for a, b in quad)

    def run_step(k, sent, w_in, w_out, y_old, y_new):
        arrive_cols(k, sent)
        step(k, w_in, w_out, y_old, y_new, 1, False)
        arrive_rows(k, sent)
        following = copies(k + 1)
        for side in range(2):
            step(k, w_in, w_out, y_old, y_new, 2 * side, True)
            send_rows(following, k + 1, side)
        return following

    sent0 = first_exchange()
    sent1 = run_step(0, sent0, w0, w1, None, y0)
    send_cols(sent1, 1, w1)
    sent2 = run_step(1, sent1, w1, w2, y0, y1)
    send_cols(sent2, 2, w2)
    sent3 = run_step(2, sent2, w2, w3, y1, y2)

    local = jnp.zeros((8, 128), F32)
    for p in range(n_pairs):
        stacked = jnp.zeros((8, 128), F32)
        for q in range(6):
            stacked = jnp.where(subl == q, jnp.sum(dots[q, p], axis=0, keepdims=True), stacked)
        for par in range(2):
            half = jnp.where(low_half, stacked, 0.0) if par == 0 else jnp.where(low_half, 0.0, stacked)
            local = jnp.where(lane == 2 * p + par, jnp.sum(half, axis=1, keepdims=True), local)

    def phase_start(i, value, size, pos, member):
        red[i, pos] = value
        moves = [
            pltpu.make_async_remote_copy(
                src_ref=red.at[i, pos],
                dst_ref=red.at[i, pos],
                send_sem=rs_send.at[i, d - 1],
                recv_sem=rs_recv.at[i, d - 1],
                device_id=member(d),
                device_id_type=MESH,
            )
            for d in range(1, size)
        ]
        for move in moves:
            move.start()
        return moves

    def phase_end(i, size, moves):
        for move in moves:
            move.wait_recv()
        return total(red[i, j] for j in range(size))

    def run_natural(slot, planes):
        for p in range(n_pairs):
            to_natural(slot, planes, p)

    moves_a = phase_start(0, local, n_zc, zc_pos, a_member)
    send_cols(sent3, 3, w3)
    for slot, planes in enumerate((y0, y1, y2)):
        run_natural(slot, planes)
    moves_b = phase_start(1, phase_end(0, n_zc, moves_a), b_size, b_pos, b_member)
    for slot, planes in enumerate((w0, w1, w2)):
        run_natural(3 + slot, planes)
    arrive_cols(3, sent3)
    arrive_rows(3, sent3)

    def last_fix(t, carry):
        r0 = pl.multiple_of(t * 8, 8)
        for p in range(n_pairs):
            value = fixed(w3, p, r0, True)
            for a, b in quad:
                w3[p, a, b, pl.ds(r0, 8), :] = value[a][b]
        return carry

    lax.fori_loop(0, 3, last_fix, 0)
    run_natural(6, w3)
    for group in (sent0, sent1, sent2, sent3, moves_a, moves_b):
        for copy in group:
            copy.wait_send()
    g = phase_end(1, b_size, moves_b)

    b0, k00, k01, k11, k12, k22 = (g[q : q + 1, :] for q in range(6))
    k02 = k11
    b1 = k00 - b0
    b2 = k01 - b1
    l10 = k01 / k00
    l20 = k02 / k00
    d1 = k11 - l10 * k01
    e12 = k12 - l10 * k02
    l21 = e12 / d1
    d2 = k22 - l20 * k02 - l21 * e12
    c1 = b1 - l10 * b0
    c2 = b2 - l20 * b0 - l21 * c1
    a2 = c2 / d2
    a1 = c1 / d1 - l21 * a2
    a0 = b0 / k00 - l10 * a1 - l20 * a2

    for m in range(n_modes):
        u0, u1, u2 = (jnp.broadcast_to(v[:, m : m + 1], (8, 128)) for v in (a0, a1, a2))
        for h in range(2):
            for a in range(4):
                for t in range(3):
                    src = pl.ds(24 * a + 8 * t, 8)
                    dst = pl.ds(a + 32 * t, 8, stride=4)
                    n = [nat[i, m, h, src, :] for i in range(7)]
                    x_ref[m, h, dst, :] = u0 * n[0] + u1 * n[1] + u2 * n[2]
                    r_ref[m, h, dst, :] = n[3] - u0 * n[4] - u1 * n[5] - u2 * n[6]


def solution(mesh, n_zc=None):
    n_curve, n_sub = mesh.shape["curve"], mesh.shape["sub"]
    n_zc = n_zc or 16
    n_y = n_curve // n_zc

    def step(forcing, metric, jacobian, mode_scale):
        n_modes, n_rows, n_cols = forcing.shape
        n_pairs = n_modes // 2
        vec = pltpu.VMEM((n_pairs, 4, 4, 24, 128), F32)
        dma = pltpu.SemaphoreType.DMA
        cfg = (n_modes, n_curve, n_sub, n_zc)
        out = jax.ShapeDtypeStruct((n_modes, 2, n_rows, 128), F32)
        slots = max(n_zc, n_y * n_sub)
        outs = pl.pallas_call(
            functools.partial(kernel, cfg),
            out_shape=(out, out),
            in_specs=[pl.BlockSpec(memory_space=pltpu.HBM)] * 4,
            out_specs=(pl.BlockSpec(memory_space=pltpu.VMEM),) * 2,
            scratch_shapes=[
                pltpu.SMEM((n_modes,), F32),
                pltpu.VMEM((n_modes, 2, n_rows, 128), F32),
                pltpu.VMEM((2, n_rows, 128), F32),
                pltpu.VMEM((2, n_rows, 128), F32),
                pltpu.VMEM((n_pairs + 1, 4, 4, 24, 128), F32),
                vec, vec, vec, vec, vec, vec, vec,
                pltpu.VMEM((7, n_modes, 2, n_rows, 128), F32),
                pltpu.VMEM((4, 4, 24, 128), F32),
                pltpu.VMEM((6, 4, 24, 128), F32),
                pltpu.VMEM((6, 4, 24, 128), F32),
                pltpu.VMEM((4, 256, 256), jnp.bfloat16),
                pltpu.VMEM((2, 2, 16, 128), F32),
                pltpu.VMEM((6, n_pairs, 8, 128), F32),
                pltpu.VMEM((4, 2, 32, 128), F32),
                pltpu.VMEM((4, 2, 8, 128), F32),
                pltpu.VMEM((4, 24, 128), F32),
                pltpu.VMEM((4, 2, 32, 128), F32),
                pltpu.VMEM((4, 4, 8, 128), F32),
                pltpu.VMEM((4, 2, 24, 128), F32),
                pltpu.VMEM((2, 32, 128), F32),
                pltpu.VMEM((24, 128), F32),
                pltpu.VMEM((2, slots, 8, 128), F32),
                dma((3 + n_modes, 2)),
                dma((4, 8)),
                dma((4, 8)),
                dma((2, slots)),
                dma((2, slots)),
            ],
            compiler_params=pltpu.CompilerParams(
                collective_id=0, has_side_effects=True, vmem_limit_bytes=VMEM_LIMIT
            ),
        )(
            *(
                pltpu.with_memory_space_constraint(v, pltpu.HBM)
                for v in (mode_scale, forcing, metric, jacobian)
            )
        )
        return tuple(jnp.swapaxes(o, 1, 2).reshape(forcing.shape) for o in outs)

    return jax.shard_map(
        step,
        mesh=mesh,
        in_specs=(P(None, "curve", "sub"), P("curve", "sub"), P("curve", "sub"), P()),
        out_specs=(P(None, "curve", "sub"), P(None, "curve", "sub")),
        check_vma=False,
    )
```

```python
import functools
import math

import jax
import jax.numpy as jnp
import numpy as np
from jax import lax
from jax.experimental import pallas as pl
from jax.experimental.pallas import tpu as pltpu
from jax.sharding import PartitionSpec as P

MESH = pl.DeviceIdType.MESH
EDGES = ((0, 1), (0, 2), (0, 3), (1, 2), (1, 3), (2, 3))
F32 = jnp.float32
VMEM_LIMIT = 40 * 1024 * 1024


def gll_slopes():
    points = np.array([-1.0, -1.0 / math.sqrt(5.0), 1.0 / math.sqrt(5.0), 1.0])
    factor = np.array(
        [np.prod([points[j] - points[m] for m in range(4) if m != j]) for j in range(4)]
    )
    slopes = np.zeros((4, 4))
    for i in range(4):
        for j in range(4):
            if i != j:
                slopes[i, j] = factor[i] / (factor[j] * (points[i] - points[j]))
        slopes[i, i] = sum((1.0 / (points[i] - points[m]) for m in range(4) if m != i))
    return slopes


def kernel(
    cfg,
    scale_hbm,
    f_hbm,
    met_hbm,
    jac_hbm,
    x_ref,
    r_ref,
    scale_ref,
    fbuf,
    metbuf,
    jacbuf,
    w0,
    w1,
    w2,
    w3,
    y0,
    y1,
    y2,
    minv,
    nat,
    mass,
    cx,
    cy,
    perm,
    edge,
    dots,
    rowbuf,
    cornbuf,
    colbuf,
    rowrecv,
    cornrecv,
    colrecv,
    rowfix,
    colfix,
    red,
    in_sems,
    send_sems,
    recv_sems,
    rs_send,
    rs_recv,
):
    n_modes, n_curve, n_sub, n_zc = cfg
    n_pairs = n_modes // 2
    n_y = n_curve // n_zc
    c = lax.axis_index("curve")
    s = lax.axis_index("sub")
    c_prev, c_next = lax.rem(c + n_curve - 1, n_curve), lax.rem(c + 1, n_curve)
    s_prev, s_next = lax.rem(s + n_sub - 1, n_sub), lax.rem(s + 1, n_sub)
    y_pos, zc_pos = c // n_zc, lax.rem(c, n_zc)
    b_size = n_y * n_sub
    b_pos = y_pos * n_sub + s

    halves = (pl.ds(0, 128), pl.ds(128, 128))
    loads = []
    for h in range(2):
        loads.append(pltpu.make_async_copy(met_hbm.at[:, halves[h]], metbuf.at[h], in_sems.at[0, h]))
        loads.append(pltpu.make_async_copy(jac_hbm.at[:, halves[h]], jacbuf.at[h], in_sems.at[1, h]))
    for m in range(n_modes):
        for h in range(2):
            loads.append(
                pltpu.make_async_copy(f_hbm.at[m, :, halves[h]], fbuf.at[m, h], in_sems.at[2 + m, h])
            )
    loads.append(pltpu.make_async_copy(scale_hbm, scale_ref, in_sems.at[2 + n_modes, 0]))
    for load in loads:
        load.start()

    def a_member(d):
        pos = lax.rem(zc_pos + d, n_zc)
        return (y_pos * n_zc + pos, s)

    def b_member(d):
        pos = lax.rem(b_pos + d, b_size)
        return ((pos // n_sub) * n_zc + zc_pos, lax.rem(pos, n_sub))

    around = [
        (c_prev, s), (c_next, s), (c, s_prev), (c, s_next),
        (c_prev, s_prev), (c_prev, s_next), (c_next, s_prev), (c_next, s_next),
    ]
    partners = around + [a_member(d) for d in range(1, n_zc)] + [b_member(d) for d in range(1, b_size)]
    barrier = pltpu.get_barrier_semaphore()
    for device in partners:
        pl.semaphore_signal(barrier, inc=1, device_id=device, device_id_type=MESH)

    def lanes_of(rows):
        return lax.broadcasted_iota(jnp.int32, (rows, 128), 1)

    def rows_of(rows):
        return lax.broadcasted_iota(jnp.int32, (rows, 128), 0)

    lane, subl = lanes_of(8), rows_of(8)
    at_low, at_high, low_half = (lane & 63) == 0, (lane & 63) == 63, lane < 64
    slopes = gll_slopes()
    weights = (1.0 / 6.0, 5.0 / 6.0, 5.0 / 6.0, 1.0 / 6.0)

    big_r = lax.broadcasted_iota(jnp.int32, (256, 256), 0)
    big_c = lax.broadcasted_iota(jnp.int32, (256, 256), 1)
    for odd in range(2):
        into = ((big_r & 3) ^ odd) * 64 + (big_r >> 2) == big_c
        perm[odd] = jnp.where(into, 1.0, 0.0).astype(jnp.bfloat16)

    def select_exact(x, which):
        high = x.astype(jnp.bfloat16)
        rest = x - high.astype(F32)
        mid = rest.astype(jnp.bfloat16)
        low = (rest - mid.astype(F32)).astype(jnp.bfloat16)
        matrix = perm[which]

        def dot(part):
            return jnp.dot(part, matrix, preferred_element_type=F32)

        return (dot(high) + dot(mid)) + dot(low)

    def natural(buf):
        return jnp.concatenate(
            [
                jnp.concatenate([buf[h, pl.ds(a, 24, stride=4), :] for a in range(4)], axis=0)
                for h in range(2)
            ],
            axis=1,
        )

    def deinterleave(x_even, x_odd):
        lo = lanes_of(x_even.shape[0]) < 64
        even, odd = select_exact(x_even, 0), select_exact(x_odd, 1)
        out = []
        for q in range(2):
            e, o = even[:, 128 * q : 128 * (q + 1)], odd[:, 128 * q : 128 * (q + 1)]
            out.append(jnp.where(lo, e, o))
            out.append(pltpu.roll(jnp.where(lo, o, e), 64, 1))
        return out

    def to_natural(slot, planes, p):
        lo = lanes_of(96) < 64
        full = [jnp.concatenate([planes[p, a, b] for a in range(4)], axis=0) for b in range(4)]
        odd1, odd3 = pltpu.roll(full[1], 64, 1), pltpu.roll(full[3], 64, 1)
        even = jnp.concatenate([jnp.where(lo, full[0], odd1), jnp.where(lo, full[2], odd3)], axis=1)
        odd = jnp.concatenate([jnp.where(lo, odd1, full[0]), jnp.where(lo, odd3, full[2])], axis=1)
        for par, packed in enumerate((even, odd)):
            out = select_exact(packed, 2 + par)
            for h in range(2):
                nat[slot, 2 * p + par, h] = out[:, 128 * h : 128 * (h + 1)]

    for load in loads[:4]:
        load.wait()
    for target, buf in ((mass, jacbuf), (minv, metbuf)):
        x = natural(buf)
        for b, plane in enumerate(deinterleave(x, x)):
            for a in range(4):
                grid_w = F32(weights[a]) * F32(weights[b])
                value = plane[24 * a : 24 * (a + 1)] * grid_w
                if target is mass:
                    mass[a, b] = value
                else:
                    minv[0, a, b] = value

    def setup(t, carry):
        rows = pl.ds(pl.multiple_of(t * 8, 8), 8)
        flux = [[minv[0, a, b, rows, :] for b in range(4)] for a in range(4)]

        def mix(values, table):
            total = values[0] * F32(table[0])
            for q in range(1, 4):
                total = total + values[q] * F32(table[q])
            return total

        for b in range(4):
            column = [flux[q][b] for q in range(4)]
            for e, (i, j) in enumerate(EDGES):
                table = slopes[:, i] * slopes[:, j]
                cx[e, b, rows, :] = mix(column, table)
                cy[e, b, rows, :] = mix(flux[b], table)
            for a in range(4):
                lap = mix(column, slopes[:, a] ** 2) + mix(flux[a], slopes[:, b] ** 2)
                w0[n_pairs, a, b, rows, :] = jnp.where(low_half, mass[a, b, rows, :], lap)
        return carry

    lax.fori_loop(0, 3, setup, 0)
    dots[...] = jnp.zeros_like(dots)
    rowbuf[...] = jnp.zeros_like(rowbuf)
    cornbuf[...] = jnp.zeros_like(cornbuf)

    lane24, row24 = lanes_of(24), rows_of(24)
    low_end = (lane24 & 63) == 0
    pack_key = ((lane24 + 1) & 63) >> 1
    pack_key2 = ((lane24 + 1) & 127) >> 1

    def row_join(w, p):
        for b in range(4):
            top, bottom = w[p, 0, b], w[p, 3, b]
            w[p, 3, b] = bottom + jnp.where(row24 < 23, pltpu.roll(top, 23, 0), 0.0)
            w[p, 0, b] = top + jnp.where(row24 > 0, pltpu.roll(bottom, 1, 0), 0.0)

    def col_join(w, p):
        inner_high, inner_low = lane24 & 63 != 63, lane24 & 63 != 0
        for a in range(4):
            first, last = w[p, a, 0], w[p, a, 3]
            w[p, a, 3] = last + jnp.where(inner_high, pltpu.roll(first, 127, 1), 0.0)
            w[p, a, 0] = first + jnp.where(inner_low, pltpu.roll(last, 1, 1), 0.0)

    def pack_cols(w, p, packed):
        for a in range(4):
            k = 4 * p + a
            ends = jnp.where(low_end, w[p, a, 0], w[p, a, 3])
            ends = pltpu.roll(ends, 2 * k, 1) if k else ends
            packed = jnp.where(pack_key == k, ends, packed)
        return packed

    def put_row(e, side, p, lines):
        for b in range(4):
            rowbuf[e, side, 8 * b + p : 8 * b + p + 1, :] = lines[b]

    def put_corners(e, side):
        cornbuf[e, side] = jnp.where(at_low, rowbuf[e, side, 0:8, :], rowbuf[e, side, 24:32, :])

    def copies(e):
        plan = [
            (rowbuf.at[e, 1], rowrecv.at[e, 0], (c_next, s)),
            (rowbuf.at[e, 0], rowrecv.at[e, 1], (c_prev, s)),
            (colbuf.at[e], colrecv.at[e, 0], (c, s_next)),
            (colbuf.at[e], colrecv.at[e, 1], (c, s_prev)),
            (cornbuf.at[e, 1], cornrecv.at[e, 0], (c_next, s_next)),
            (cornbuf.at[e, 1], cornrecv.at[e, 1], (c_next, s_prev)),
            (cornbuf.at[e, 0], cornrecv.at[e, 2], (c_prev, s_next)),
            (cornbuf.at[e, 0], cornrecv.at[e, 3], (c_prev, s_prev)),
        ]
        return [
            pltpu.make_async_remote_copy(
                src_ref=src,
                dst_ref=dst,
                send_sem=send_sems.at[e, i],
                recv_sem=recv_sems.at[e, i],
                device_id=device,
                device_id_type=MESH,
            )
            for i, (src, dst, device) in enumerate(plan)
        ]

    def send_rows(sent, e, side):
        put_corners(e, side)
        for i in (6, 7, 1) if side == 0 else (4, 5, 0):
            sent[i].start()

    def send_cols(sent, e, w):
        packed = jnp.zeros((24, 128), F32)
        for p in range(n_pairs):
            row_join(w, p)
            packed = pack_cols(w, p, packed)
        colbuf[e] = packed
        for copy in sent[2:4]:
            copy.start()
        for p in range(n_pairs):
            col_join(w, p)

    def first_exchange():
        sent = copies(0)
        edge[...] = jnp.zeros_like(edge)
        for load in loads[4:-1]:
            load.wait()
        for m in range(n_modes):
            for h in range(2):
                for side in range(2):
                    r, i = 8 * side + m // 2, 95 * side
                    edge[m % 2, h, r : r + 1, :] = fbuf[m, h, i : i + 1, :]
        planes = deinterleave(
            *(jnp.concatenate([edge[par, 0], edge[par, 1]], axis=1) for par in range(2))
        )
        for side in range(2):
            for b in range(4):
                line = mass[0, b, 0:1, :] if side == 0 else mass[3, b, 23:24, :]
                rowbuf[0, side, 8 * b : 8 * b + 8, :] = planes[b][8 * side : 8 * side + 8] * line
        put_row(0, 0, n_pairs, [w0[n_pairs, 0, b, 0:1, :] for b in range(4)])
        put_row(0, 1, n_pairs, [w0[n_pairs, 3, b, 23:24, :] for b in range(4)])
        pl.semaphore_wait(barrier, len(partners))
        send_rows(sent, 0, 0)
        send_rows(sent, 0, 1)
        packed = jnp.zeros((24, 128), F32)
        for a in range(4):
            every = pl.ds(a, 24, stride=4)
            grid_w = F32(weights[a]) * F32(weights[0])
            ends_mass = jnp.where(lane24 == 127, jacbuf[1, every, :], jacbuf[0, every, :]) * grid_w
            for p in range(n_pairs):
                for par in range(2):
                    k = 4 * p + a + 32 * par
                    ends = jnp.where(
                        lane24 == 127, fbuf[2 * p + 1 - par, 1, every, :], fbuf[2 * p + par, 0, every, :]
                    )
                    ends = ends * ends_mass
                    ends = pltpu.roll(ends, 2 * k, 1) if k else ends
                    packed = jnp.where(pack_key2 == k, ends, packed)
        below = pltpu.roll(pltpu.roll(packed, 6, 1), 23, 0)
        above = pltpu.roll(pltpu.roll(packed, 122, 1), 1, 0)
        packed = (
            packed
            + jnp.where(((pack_key & 3) == 3) & (row24 < 23), below, 0.0)
            + jnp.where(((pack_key & 3) == 0) & (row24 > 0), above, 0.0)
        )
        row_join(w0, n_pairs)
        colbuf[0] = pack_cols(w0, n_pairs, packed)
        for copy in sent[2:4]:
            copy.start()
        for p in range(n_pairs):
            planes = deinterleave(natural(fbuf.at[2 * p]), natural(fbuf.at[2 * p + 1]))
            for b in range(4):
                for a in range(4):
                    w0[p, a, b] = planes[b][24 * a : 24 * (a + 1)] * mass[a, b]
            row_join(w0, p)
            col_join(w0, p)
        col_join(w0, n_pairs)
        for odd in range(2):
            back = ((big_c & 3) ^ odd) * 64 + (big_c >> 2) == big_r
            perm[2 + odd] = jnp.where(back, 1.0, 0.0).astype(jnp.bfloat16)
        loads[-1].wait()
        return sent

    def arrive_cols(e, sent):
        for copy in sent[2:4]:
            copy.wait_recv()
        colfix[...] = jnp.where(
            (lane24 & 1) == 0, pltpu.roll(colrecv[e, 0], 65, 1), pltpu.roll(colrecv[e, 1], 63, 1)
        )

    def arrive_rows(e, sent):
        for copy in sent[:2] + sent[4:]:
            copy.wait_recv()
        for side in range(2):
            r = [rowrecv[e, side, 8 * b : 8 * b + 8, :] for b in range(4)]
            left = pltpu.roll(cornrecv[e, 2 * side], 65, 1)
            right = pltpu.roll(cornrecv[e, 2 * side + 1], 63, 1)
            rowfix[side, 0:8, :] = r[0] + jnp.where(at_low, left, pltpu.roll(r[3], 1, 1))
            rowfix[side, 8:16, :] = r[1]
            rowfix[side, 16:24, :] = r[2]
            rowfix[side, 24:32, :] = r[3] + jnp.where(at_high, right, pltpu.roll(r[0], 127, 1))

    def fixed(w, p, r0, outer):
        rows = pl.ds(r0, 8)
        out = []
        for a in range(4):
            k = 4 * p + a
            ends = colfix[rows, :]
            ends = pltpu.roll(ends, (-2 * k) % 128, 1) if k else ends
            line = []
            for b in range(4):
                value = w[p, a, b, rows, :]
                if b == 0:
                    value = value + jnp.where(at_low, ends, 0.0)
                if b == 3:
                    value = value + jnp.where(at_high, ends, 0.0)
                r = 8 * b + p
                if outer and a == 0:
                    value = value + jnp.where(subl + r0 == 0, rowfix[0, r : r + 1, :], 0.0)
                if outer and a == 3:
                    value = value + jnp.where(subl + r0 == 23, rowfix[1, r : r + 1, :], 0.0)
                line.append(value)
            out.append(line)
        return out

    def total(values):
        values = list(values)
        while len(values) > 1:
            values = [
                values[i] + values[i + 1] if i + 1 < len(values) else values[i]
                for i in range(0, len(values), 2)
            ]
        return values[0]

    quad = [(a, b) for a in range(4) for b in range(4)]

    def step(k, w_in, w_out, y_old, y_new, t, outer):
        r0 = 8 * t
        rows = pl.ds(r0, 8)
        if k == 0:
            both = fixed(w_in, n_pairs, r0, outer)
            for a, b in quad:
                swapped = pltpu.roll(both[a][b], 64, 1)
                w_in[n_pairs, a, b, rows, :] = jnp.where(low_half, both[a][b], swapped)
                y2[0, a, b, rows, :] = jnp.where(low_half, swapped, both[a][b])
        for p in range(n_pairs):
            scale = jnp.where(low_half, scale_ref[2 * p], scale_ref[2 * p + 1])
            value = fixed(w_in, p, r0, outer)
            vec = [[None] * 4 for _ in range(4)]
            for a, b in quad:
                w_in[p, a, b, rows, :] = value[a][b]
                if k == 0:
                    diag = w_in[n_pairs, a, b, rows, :] + scale * y2[0, a, b, rows, :]
                    inv = 1.0 / diag
                    minv[p, a, b, rows, :] = inv
                    vec[a][b] = value[a][b] * inv
                else:
                    vec[a][b] = value[a][b] * minv[p, a, b, rows, :] - y_old[p, a, b, rows, :]
                y_new[p, a, b, rows, :] = vec[a][b]
            lap = [[None] * 4 for _ in range(4)]

            def flow(table, e, line, i, j):
                (ai, bi), (aj, bj) = i, j
                f = table[e, line, rows, :] * (vec[aj][bj] - vec[ai][bi])
                lap[ai][bi] = f if lap[ai][bi] is None else lap[ai][bi] + f
                lap[aj][bj] = -f if lap[aj][bj] is None else lap[aj][bj] - f

            for line in range(4):
                for e, (i, j) in enumerate(EDGES):
                    flow(cx, e, line, (i, line), (j, line))
            image = [[None] * 4 for _ in range(4)]
            for a in range(4):
                for e, (i, j) in enumerate(EDGES):
                    flow(cy, e, a, (a, i), (a, j))
                for b in range(4):
                    image[a][b] = mass[a, b, rows, :] * vec[a][b] + scale * lap[a][b]
                    w_out[p, a, b, rows, :] = image[a][b]
            if outer:
                side = t // 2
                put_row(k + 1, side, p, [image[3 * side][b][7 * side : 7 * side + 1] for b in range(4)])
            if k == 0:
                count = (0.5, 1.0, 1.0, 0.5)
                terms = []
                for a, b in quad:
                    term = vec[a][b] * value[a][b]
                    weight = count[a] * count[b]
                    terms.append(term if weight == 1.0 else term * F32(weight))
                dots[0, p] += total(terms)
                dots[1, p] += total(vec[a][b] * image[a][b] for a, b in quad)
            else:
                dots[2 * k, p] += total(y_old[p, a, b, rows, :] * image[a][b] for a, b in quad)
                dots[2 * k + 1, p] += total(vec[a][b] * image[a][b] for a, b in quad)

    def run_step(k, sent, w_in, w_out, y_old, y_new):
        arrive_cols(k, sent)
        step(k, w_in, w_out, y_old, y_new, 1, False)
        arrive_rows(k, sent)
        following = copies(k + 1)
        for side in range(2):
            step(k, w_in, w_out, y_old, y_new, 2 * side, True)
            send_rows(following, k + 1, side)
        return following

    def gather_dots(first, last):
        local = jnp.zeros((8, 128), F32)
        for p in range(n_pairs):
            stacked = jnp.zeros((8, 128), F32)
            for q in range(first, last):
                stacked = jnp.where(subl == q, jnp.sum(dots[q, p], axis=0, keepdims=True), stacked)
            for par in range(2):
                half = jnp.where(low_half, stacked, 0.0) if par == 0 else jnp.where(low_half, 0.0, stacked)
                local = jnp.where(lane == 2 * p + par, jnp.sum(half, axis=1, keepdims=True), local)
        return local

    sent0 = first_exchange()
    sent1 = run_step(0, sent0, w0, w1, None, y0)
    send_cols(sent1, 1, w1)
    sent2 = run_step(1, sent1, w1, w2, y0, y1)
    send_cols(sent2, 2, w2)
    early = gather_dots(0, 4)
    sent3 = run_step(2, sent2, w2, w3, y1, y2)

    def phase_start(i, value, size, pos, member):
        red[i, pos] = value
        moves = [
            pltpu.make_async_remote_copy(
                src_ref=red.at[i, pos],
                dst_ref=red.at[i, pos],
                send_sem=rs_send.at[i, d - 1],
                recv_sem=rs_recv.at[i, d - 1],
                device_id=member(d),
                device_id_type=MESH,
            )
            for d in range(1, size)
        ]
        for move in moves:
            move.start()
        return moves

    def phase_end(i, size, moves):
        for move in moves:
            move.wait_recv()
        return total(red[i, j] for j in range(size))

    def run_natural(slot, planes):
        for p in range(n_pairs):
            to_natural(slot, planes, p)

    moves_a = phase_start(0, early + gather_dots(4, 6), n_zc, zc_pos, a_member)
    send_cols(sent3, 3, w3)
    for slot, planes in enumerate((y0, y1, y2)):
        run_natural(slot, planes)
    moves_b = phase_start(1, phase_end(0, n_zc, moves_a), b_size, b_pos, b_member)
    for slot, planes in enumerate((w0, w1, w2)):
        run_natural(3 + slot, planes)
    arrive_cols(3, sent3)
    arrive_rows(3, sent3)

    def last_fix(t, carry):
        r0 = pl.multiple_of(t * 8, 8)
        for p in range(n_pairs):
            value = fixed(w3, p, r0, True)
            for a, b in quad:
                w3[p, a, b, pl.ds(r0, 8), :] = value[a][b]
        return carry

    lax.fori_loop(0, 3, last_fix, 0)
    run_natural(6, w3)
    g = phase_end(1, b_size, moves_b)

    b0, k00, k01, k11, k12, k22 = (g[q : q + 1, :] for q in range(6))
    k02 = k11
    b1 = k00 - b0
    b2 = k01 - b1
    l10 = k01 / k00
    l20 = k02 / k00
    d1 = k11 - l10 * k01
    e12 = k12 - l10 * k02
    l21 = e12 / d1
    d2 = k22 - l20 * k02 - l21 * e12
    c1 = b1 - l10 * b0
    c2 = b2 - l20 * b0 - l21 * c1
    a2 = c2 / d2
    a1 = c1 / d1 - l21 * a2
    a0 = b0 / k00 - l10 * a1 - l20 * a2

    for m in range(n_modes):
        u0, u1, u2 = (jnp.broadcast_to(v[:, m : m + 1], (8, 128)) for v in (a0, a1, a2))
        for h in range(2):
            for a in range(4):
                for t in range(3):
                    src = pl.ds(24 * a + 8 * t, 8)
                    dst = pl.ds(a + 32 * t, 8, stride=4)
                    n = [nat[i, m, h, src, :] for i in range(7)]
                    x_ref[m, h, dst, :] = u0 * n[0] + u1 * n[1] + u2 * n[2]
                    r_ref[m, h, dst, :] = n[3] - u0 * n[4] - u1 * n[5] - u2 * n[6]
    for group in (sent0, sent1, sent2, sent3, moves_a, moves_b):
        for copy in group:
            copy.wait_send()


def solution(mesh, n_zc=None):
    n_curve, n_sub = mesh.shape["curve"], mesh.shape["sub"]
    n_zc = n_zc or 16
    n_y = n_curve // n_zc

    def step(forcing, metric, jacobian, mode_scale):
        n_modes, n_rows, n_cols = forcing.shape
        n_pairs = n_modes // 2
        vec = pltpu.VMEM((n_pairs, 4, 4, 24, 128), F32)
        dma = pltpu.SemaphoreType.DMA
        cfg = (n_modes, n_curve, n_sub, n_zc)
        out = jax.ShapeDtypeStruct((n_modes, 2, n_rows, 128), F32)
        slots = max(n_zc, n_y * n_sub)
        outs = pl.pallas_call(
            functools.partial(kernel, cfg),
            out_shape=(out, out),
            in_specs=[pl.BlockSpec(memory_space=pltpu.HBM)] * 4,
            out_specs=(pl.BlockSpec(memory_space=pltpu.VMEM),) * 2,
            scratch_shapes=[
                pltpu.SMEM((n_modes,), F32),
                pltpu.VMEM((n_modes, 2, n_rows, 128), F32),
                pltpu.VMEM((2, n_rows, 128), F32),
                pltpu.VMEM((2, n_rows, 128), F32),
                pltpu.VMEM((n_pairs + 1, 4, 4, 24, 128), F32),
                vec, vec, vec, vec, vec, vec, vec,
                pltpu.VMEM((7, n_modes, 2, n_rows, 128), F32),
                pltpu.VMEM((4, 4, 24, 128), F32),
                pltpu.VMEM((6, 4, 24, 128), F32),
                pltpu.VMEM((6, 4, 24, 128), F32),
                pltpu.VMEM((4, 256, 256), jnp.bfloat16),
                pltpu.VMEM((2, 2, 16, 128), F32),
                pltpu.VMEM((6, n_pairs, 8, 128), F32),
                pltpu.VMEM((4, 2, 32, 128), F32),
                pltpu.VMEM((4, 2, 8, 128), F32),
                pltpu.VMEM((4, 24, 128), F32),
                pltpu.VMEM((4, 2, 32, 128), F32),
                pltpu.VMEM((4, 4, 8, 128), F32),
                pltpu.VMEM((4, 2, 24, 128), F32),
                pltpu.VMEM((2, 32, 128), F32),
                pltpu.VMEM((24, 128), F32),
                pltpu.VMEM((2, slots, 8, 128), F32),
                dma((3 + n_modes, 2)),
                dma((4, 8)),
                dma((4, 8)),
                dma((2, slots)),
                dma((2, slots)),
            ],
            compiler_params=pltpu.CompilerParams(
                collective_id=0, has_side_effects=True, vmem_limit_bytes=VMEM_LIMIT
            ),
        )(
            *(
                pltpu.with_memory_space_constraint(v, pltpu.HBM)
                for v in (mode_scale, forcing, metric, jacobian)
            )
        )
        return tuple(jnp.swapaxes(o, 1, 2).reshape(forcing.shape) for o in outs)

    return jax.shard_map(
        step,
        mesh=mesh,
        in_specs=(P(None, "curve", "sub"), P("curve", "sub"), P("curve", "sub"), P()),
        out_specs=(P(None, "curve", "sub"), P(None, "curve", "sub")),
        check_vma=False,
    )
```
